32 devices in a mesh: section: 2 (over y), dp: 16 (over z, x, core).
Axes of the slice: x: 2, y: 2, z: 4, core: 2. Of those that a mesh axis runs over, the one named last changes fastest.
Arguments:
- residuals: float32 [8, 128, 4096], P('section', 'dp'), may hold values from -100 to 100, as said below
- owners: int32 [32], replicated, may hold values from 0 to 31, each once
Outputs:
- harvest: bfloat16 [128, 8, 4096], P(('section', 'dp'))
The draws below stay inside these ranges and needn't reach their ends.
Inputs may be any that keep to these rules, and one draw needn't show every extreme that they name: `owners`: a permutation of the block numbers. `residuals`: real-valued activations.
All inputs are finite; a program needn't handle non-finite values.
Results may differ from the reference program's by a relative error of at most 0.0004.
Values may be sent and summed in bfloat16 or wider, within the bound.
A program may use at most 64 MiB of HBM per device.

```python
import math
import jax
import jax.numpy as jnp
from jax import lax

D = 4096
BLOCK = 4
LAYERS = 8
TOK_DEV = 8
TOKENS = 128
BLOCKS = 32


def draw_residuals(key, part):
    noise_key = jax.random.fold_in(key, 11)
    shard_key = jax.random.fold_in(key, 12)
    token_key = jax.random.fold_in(key, 13)
    offset_key = jax.random.fold_in(key, 14)
    shard_count = TOKENS // TOK_DEV
    base_noise = jax.random.normal(noise_key, (LAYERS, TOKENS, D), jnp.float32)
    log_low = math.log(0.3)
    log_high = math.log(3.0)
    shard_scale = jnp.exp(jax.random.uniform(shard_key, (LAYERS, shard_count, 1, 1), jnp.float32, log_low, log_high))
    token_scale = jax.random.uniform(token_key, (LAYERS, TOKENS, 1), jnp.float32, 0.5, 1.5)
    offset = 2.0 * jax.random.normal(offset_key, (LAYERS, TOKENS, 1), jnp.float32)
    scaled_rows = base_noise.reshape(LAYERS, shard_count, TOK_DEV, D) * shard_scale
    return jnp.clip(scaled_rows.reshape(LAYERS, TOKENS, D) * token_scale + offset, -100.0, 100.0)


def setup_inputs(seed: int = 0) -> dict:
    key_list = jax.random.split(jax.random.key(seed), 3)
    return {
        "residuals": draw_residuals(jax.random.fold_in(key_list[2], 71), 0),
        "owners": jax.random.permutation(key_list[1], BLOCKS).astype(jnp.int32),
    }


def reference(residuals, owners):

    def normalize_layer(layer_rows):
        centered = layer_rows - lax.optimization_barrier(jnp.mean(layer_rows, axis=1, keepdims=True))
        energy = jnp.sum(centered * centered)
        layer_scale = 1.0 / jnp.sqrt(energy / (TOKENS * D) + 1.0)
        return (centered * layer_scale).astype(jnp.bfloat16)
    normed = lax.map(normalize_layer, residuals)
    inverse = jnp.zeros((BLOCKS,), jnp.int32).at[owners.astype(jnp.int32)].set(jnp.arange(BLOCKS, dtype=jnp.int32))
    blocked = normed.reshape(LAYERS, BLOCKS, BLOCK, D)[:, inverse]
    return blocked.transpose(1, 2, 0, 3).reshape(TOKENS, LAYERS, D)
```

```python
import functools

import jax
import jax.numpy as jnp
from jax import lax
from jax.experimental import pallas as pl
from jax.experimental.pallas import tpu as pltpu
from jax.sharding import PartitionSpec as P

MESH = pl.DeviceIdType.MESH
LANES = 128
SUBLANES = 8
QUARTERS = 4
EARLY = 2
LAG = 8


def harvest_kernel(sections, groups, planes, units, early, x_hbm, owners_hbm, out_ref, owners, inverse, xv, centered,
                   part, part2, parts, s1, s2, r2, x_sem, o_sem, e_send, e_recv, r_recv, below, above, send1, recv1,
                   send2, recv2, *r1):
    layers, tokens, features = x_hbm.shape
    blocks = s2.shape[1]
    per_dev = blocks // groups
    chunks = features // groups // LANES
    width = features // groups
    plane = groups // planes
    section, group = lax.axis_index("section"), lax.axis_index("dp")
    me = section * groups + group
    z, place = group // plane, lax.rem(group, plane)

    load = pltpu.make_async_copy(x_hbm, xv, x_sem)
    load.start()
    load_owners = pltpu.make_async_copy(owners_hbm, owners, o_sem)
    load_owners.start()
    barrier = pltpu.get_barrier_semaphore()

    def at(t, k):
        return (z + t) * plane + lax.rem(place + k, plane)

    def when(t, body):
        if t == 0:
            body()
        elif t > 0:
            pl.when(z < planes - t)(body)
        else:
            pl.when(z >= -t)(body)

    def peers(t):
        return range(1 if t == 0 else 0, plane)

    near = [t for t in (0, 1, -1) if abs(t) < planes]
    for t in near:
        @functools.partial(when, t)
        def _():
            for k in peers(t):
                pl.semaphore_signal(barrier, inc=1, device_id=(section, at(t, k)), device_id_type=MESH)
    for k in range(1, sections):
        pl.semaphore_signal(barrier, inc=1, device_id=(lax.rem(section + k, sections), group), device_id_type=MESH)

    load.wait()
    per_tile = SUBLANES // layers
    lane = lax.broadcasted_iota(jnp.int32, (SUBLANES, LANES), 1)
    row = lax.broadcasted_iota(jnp.int32, (SUBLANES, LANES), 0)
    total = jnp.zeros((SUBLANES, LANES), jnp.float32)
    for l in range(layers):
        acc = jnp.zeros((SUBLANES, LANES), jnp.float32)
        for t in range(0, tokens, SUBLANES):
            x = xv[l, t:t + SUBLANES]
            c = x - jnp.sum(x, axis=1, keepdims=True) * (1.0 / features)
            xv[l, t:t + SUBLANES] = c
            sq = c * c
            for f in range(features // LANES):
                acc = acc + sq[:, f * LANES:(f + 1) * LANES]
        fold = LANES // 2
        while fold >= LANES // layers:
            acc = acc + pltpu.roll(acc, fold, 1)
            fold //= 2
        total = total + jnp.where(lane // (LANES // layers) == l, acc, 0.0)
    own_lanes = lane // (LANES // layers) == row % layers
    acc = jnp.sum(total, axis=0, keepdims=True)
    part[...] = acc
    parts[group] = acc
    if planes > 3:
        @pl.when(z >= planes - 1)
        def _():
            parts[0:plane] = jnp.zeros((plane, 1, LANES), jnp.float32)

    tiles = range(tokens // per_tile)
    tiles_per_block = tokens // per_dev // per_tile

    def regroup(g):
        j, tile = divmod(g, tiles_per_block)
        c = jnp.concatenate([xv[:, g * per_tile + i, :] for i in range(per_tile)], axis=0)
        for f in range(features // LANES):
            centered[tile, f, j] = c[:, f * LANES:(f + 1) * LANES]

    early_tiles = {tile for tile, _ in units[:early]}
    first = [g for g in tiles if g % tiles_per_block in early_tiles]
    for g in first:
        regroup(g)

    mine = pl.ds(group * per_dev, per_dev)

    def send_part(source, t):
        for k in peers(t):
            pltpu.make_async_remote_copy(
                src_ref=source, dst_ref=parts.at[group], send_sem=e_send,
                recv_sem=r_recv if t == 1 and k == 0 else e_recv,
                device_id=(section, at(t, k)), device_id_type=MESH).start()

    def energies(count, sem=None):
        span = parts.at[pl.ds(0, count)]
        return pltpu.make_async_remote_copy(
            src_ref=span, dst_ref=span, send_sem=e_send, recv_sem=e_recv if sem is None else sem,
            device_id=(section, group), device_id_type=MESH)

    def relayed():
        return energies(1, r_recv)

    def send_unit(u, d, source):
        pltpu.make_async_remote_copy(
            src_ref=source, dst_ref=r1[u].at[mine], send_sem=send1.at[u], recv_sem=recv1.at[u],
            device_id=(section, d), device_id_type=MESH).start()

    def raw(u, d):
        tile, k = units[u]
        return centered.at[tile, d * chunks + k]

    def send_early(t):
        for u in range(early):
            for k in peers(t):
                send_unit(u, at(t, k), raw(u, at(t, k)))

    def neighbour(sem, t):
        pl.semaphore_signal(sem, inc=1, device_id=(section, at(t, 0)), device_id_type=MESH)

    both = (z + planes - 1) // planes + (2 * planes - 2 - z) // planes
    pl.semaphore_wait(barrier, plane * (1 + both) - 1 + sections - 1)
    for t in near:
        when(t, lambda: send_part(part, t))
    if planes > 2:
        @pl.when((z >= 1) & (z < planes - 1))
        def _():
            neighbour(below.at[2], 1)
            neighbour(above.at[2], -1)

    for t in range(2, planes):
        @functools.partial(when, -t)
        def _():
            pl.semaphore_wait(below.at[t], 1)
            if t + 1 < planes:
                when(1, lambda: neighbour(below.at[t + 1], 1))
            send_part(part, -t)

    for t in sorted([t for t in near if t] + [-t for t in range(2, planes)]):
        when(t, lambda: send_early(t))
    for t in range(2, planes):
        @functools.partial(when, t)
        def _():
            pl.semaphore_wait(above.at[t], 1)
            if t + 1 < planes:
                when(-1, lambda: neighbour(above.at[t + 1], -1))
            if t == 2:
                @pl.when(z >= 1)
                def _():
                    relayed().wait_recv()
                    part2[...] = part[...] + parts[group - plane]

                @pl.when(z < 1)
                def _():
                    part2[...] = part[...]
                send_part(part2, t)
            send_early(t)
    send_early(0)

    for g in tiles:
        if g not in first:
            regroup(g)
    load_owners.wait()

    @pl.loop(0, blocks)
    def _(o):
        found = jnp.int32(0)
        for b in range(blocks):
            found = jnp.where(owners[b] == o, jnp.int32(b), found)
        inverse[o] = found

    @pl.when(z < 1)
    def _():
        energies(groups - 1).wait_recv()

    @pl.when(z >= 1)
    def _():
        if planes <= 3:
            energies(groups - 2).wait_recv()
        else:
            @pl.when(z < planes - 1)
            def _():
                energies(groups - 2).wait_recv()

            @pl.when(z >= planes - 1)
            def _():
                energies(groups - 2 - plane).wait_recv()
        pl.when(z >= planes - 2)(lambda: relayed().wait_recv())

    total = parts[0]
    for g in range(1, groups):
        total = total + parts[g]
    energy = jnp.sum(jnp.where(own_lanes, total, 0.0), axis=1, keepdims=True)
    scale = 1.0 / jnp.sqrt(energy * (1.0 / (tokens * groups * features)) + 1.0)

    maps = [z]
    if planes > 1:
        half = lax.rem(z + 2, planes)
        maps = [planes - 1 - z, half, planes - 1 - half, z]

    def partners(m):
        return [maps[m] * plane + lax.rem(place + k, plane) for k in range(plane)]

    for u in range(early, len(units)):
        tile, k = units[u]
        for d in range(groups):
            for j in range(per_dev):
                s1[u - early, d * per_dev + j] = (centered[tile, d * chunks + k, j] * scale).astype(jnp.bfloat16)
        for m in range(len(maps)):
            for n, d in enumerate(partners(m)):
                if m < len(maps) - 1 or n:
                    send_unit(u, d, s1.at[u - early, pl.ds(d * per_dev, per_dev)])
        r1[u][mine] = s1[u - early, mine]
    for u in range(early):
        r1[u][mine] = raw(u, group)[...]

    def arrived(u):
        span = r1[u].at[pl.ds(0, (groups - 1) * per_dev)]
        return pltpu.make_async_remote_copy(
            src_ref=span, dst_ref=span, send_sem=send1.at[u], recv_sem=recv1.at[u],
            device_id=(section, group), device_id_type=MESH)

    def delivered(u):
        span = r2.at[u, pl.ds(0, sections * groups - 1)]
        return pltpu.make_async_remote_copy(
            src_ref=span, dst_ref=span, send_sem=send2.at[u], recv_sem=recv2.at[u],
            device_id=(section, group), device_id_type=MESH)

    routes = [(m, n, q) for m in range(len(maps)) for n in range(plane) for q in range(sections)]
    routes = [r for r in routes if r != (len(maps) - 1, 0, 0)] + [(len(maps) - 1, 0, 0)]

    def deliver(u):
        def spot(m, n, q):
            sec, d = lax.rem(section + q, sections), partners(m)[n]
            return sec, d, sec * groups + d

        def select(m, n, q):
            o = spot(m, n, q)[2]
            block = r1[u][inverse[o]]
            if u < early:
                block = (block * scale).astype(jnp.bfloat16)
            if (m, n, q) == routes[-1]:
                r2[u, o] = block
            else:
                s2[u, o] = block

        def send(m, n, q):
            sec, d, o = spot(m, n, q)
            pltpu.make_async_remote_copy(
                src_ref=s2.at[u, o], dst_ref=r2.at[u, me], send_sem=send2.at[u], recv_sem=recv2.at[u],
                device_id=(sec, d), device_id_type=MESH).start()

        for n in range(len(routes) + LAG):
            if n < len(routes):
                select(*routes[n])
            if LAG <= n < len(routes) - 1 + LAG:
                send(*routes[n - LAG])

    for u in range(len(units)):
        arrived(u).wait_recv()
        deliver(u)

    for u, (tile, k) in enumerate(units):
        delivered(u).wait_recv()
        for d in range(groups):
            got = [r2[u, s * groups + d].astype(jnp.float32) for s in range(sections)]
            lane = d * width + k * LANES
            for i in range(per_tile):
                out_ref[tile * per_tile + i, :, lane:lane + LANES] = jnp.concatenate(
                    [v[i * layers:(i + 1) * layers] for v in got], axis=0).astype(jnp.bfloat16)

    if planes > 3:
        @pl.when(z < 1)
        def _():
            energies(groups - 1 - plane).wait_send()

        @pl.when(z >= 1)
        def _():
            energies(groups - 1).wait_send()
    else:
        energies(groups - 1).wait_send()
    for u in range(len(units)):
        arrived(u).wait_send()
        delivered(u).wait_send()


def store_kernel(assembled, out_hbm, sem):
    store = pltpu.make_async_copy(assembled, out_hbm, sem)
    store.start()
    store.wait()


def solution(mesh):
    sections, groups = mesh.shape["section"], mesh.shape["dp"]
    planes = QUARTERS if groups % QUARTERS == 0 else 1

    def on_device(residuals, owners):
        layers, tokens, features = residuals.shape
        blocks = owners.shape[0]
        per_dev = blocks // groups
        block_len = tokens // per_dev
        chunks = features // groups // LANES
        row_tiles = block_len * layers // SUBLANES
        units = [(tile, k) for tile in range(row_tiles) for k in range(chunks)]
        early = min(EARLY, len(units) // 2)
        tile = (SUBLANES, LANES)
        dma, flag = pltpu.SemaphoreType.DMA, pltpu.SemaphoreType.REGULAR
        received = pl.pallas_call(
            functools.partial(harvest_kernel, sections, groups, planes, units, early),
            out_shape=pltpu.VMEM((block_len, layers * sections, features), jnp.bfloat16),
            in_specs=[pl.BlockSpec(memory_space=pl.ANY), pl.BlockSpec(memory_space=pl.ANY)],
            out_specs=pl.BlockSpec(memory_space=pltpu.VMEM),
            scratch_shapes=[
                pltpu.SMEM((blocks,), jnp.int32),
                pltpu.SMEM((blocks,), jnp.int32),
                pltpu.VMEM((layers, tokens, features), jnp.float32),
                pltpu.VMEM((row_tiles, features // LANES, per_dev, *tile), jnp.float32),
                pltpu.VMEM((1, LANES), jnp.float32),
                pltpu.VMEM((1, LANES), jnp.float32),
                pltpu.VMEM((groups, 1, LANES), jnp.float32),
                pltpu.VMEM((len(units) - early, blocks, *tile), jnp.bfloat16),
                pltpu.VMEM((len(units), blocks, *tile), jnp.bfloat16),
                pltpu.VMEM((len(units), blocks, *tile), jnp.bfloat16),
                dma, dma, dma, dma, dma,
                flag((QUARTERS,)), flag((QUARTERS,)),
                *[dma((len(units),)) for _ in range(4)],
                *[pltpu.VMEM((blocks, *tile), jnp.float32 if u < early else jnp.bfloat16) for u in range(len(units))],
            ],
            compiler_params=pltpu.CompilerParams(collective_id=0, has_side_effects=True),
            name="harvest",
        )(residuals, owners)
        return pl.pallas_call(
            store_kernel,
            out_shape=jax.ShapeDtypeStruct(received.shape, received.dtype),
            in_specs=[pl.BlockSpec(memory_space=pltpu.VMEM)],
            out_specs=pl.BlockSpec(memory_space=pl.ANY),
            scratch_shapes=[pltpu.SemaphoreType.DMA],
            name="store",
        )(pltpu.with_memory_space_constraint(received, pltpu.VMEM))

    in_specs = (P("section", "dp", None), P())
    out_specs = P(("section", "dp"), None, None)
    return jax.shard_map(on_device, mesh=mesh, in_specs=in_specs, out_specs=out_specs, check_vma=False)
```

```python
import functools

import jax
import jax.numpy as jnp
from jax import lax
from jax.experimental import pallas as pl
from jax.experimental.pallas import tpu as pltpu
from jax.sharding import PartitionSpec as P

MESH = pl.DeviceIdType.MESH
LANES = 128
SUBLANES = 8
LAG = 8
FULL = 1
EFIRST = 1
SPLIT = 0
LSPLIT = 0
NUNITS = 3
ORDE = 'near'
ORDL = 'near'
STEPS = ((0, (0, 2)), (1, (0, 2, 3)), (2, (0, 2, 3)), (0, (1, 3)), (1, (1,)), (2, (1,)))


def harvest_kernel(sections, groups, narrow, kinds, x_hbm, owners_hbm, out_ref, owners, inverse, xv, centered, part,
                   parts, x_sem, o_sem, e_send, e_recv, send1, recv1, send2, recv2, *buffers):
    layers, tokens, features = x_hbm.shape
    pieces = features // LANES
    blocks = owners.shape[0]
    per_dev = blocks // groups
    side, quarter = groups // 2, groups // 4
    row_tiles = centered.shape[0]
    each = sum(len(k) for k in kinds)
    wide_chunks = groups * each // row_tiles
    units = narrow + len(kinds)
    r1, s2, r2, late = buffers[:units], buffers[units:2 * units], buffers[2 * units:3 * units], buffers[3 * units:]
    section, group = lax.axis_index("section"), lax.axis_index("dp")
    me = section * groups + group
    upper = group // side
    spot, base = lax.rem(group, side), upper * side

    load = pltpu.make_async_copy(x_hbm, xv, x_sem)
    load.start()
    load_owners = pltpu.make_async_copy(owners_hbm, owners, o_sem)
    load_owners.start()
    barrier = pltpu.get_barrier_semaphore()

    def peer_of(p):
        return lax.rem(group + p, groups)

    def beside(k):
        return base + lax.rem(spot + k, side)

    def across(k):
        return side - base + lax.rem(spot + k, side)

    def signal(sem, d):
        pl.semaphore_signal(sem, inc=1, device_id=(section, d), device_id_type=MESH)

    for p in range(1, groups):
        signal(barrier, peer_of(p))
    for k in range(1, sections):
        pl.semaphore_signal(barrier, inc=1, device_id=(lax.rem(section + k, sections), group), device_id_type=MESH)

    load.wait()
    per_tile = SUBLANES // layers
    lane = lax.broadcasted_iota(jnp.int32, (SUBLANES, LANES), 1)
    row = lax.broadcasted_iota(jnp.int32, (SUBLANES, LANES), 0)
    total = jnp.zeros((SUBLANES, LANES), jnp.float32)
    for l in range(layers):
        acc = jnp.zeros((SUBLANES, LANES), jnp.float32)
        for t in range(0, tokens, SUBLANES):
            x = xv[l, t:t + SUBLANES]
            c = x - jnp.sum(x, axis=1, keepdims=True) * (1.0 / features)
            xv[l, t:t + SUBLANES] = c
            sq = c * c
            for f in range(pieces):
                acc = acc + sq[:, f * LANES:(f + 1) * LANES]
        fold = LANES // 2
        while fold >= LANES // layers:
            acc = acc + pltpu.roll(acc, fold, 1)
            fold //= 2
        total = total + jnp.where(lane // (LANES // layers) == l, acc, 0.0)
    own_lanes = lane // (LANES // layers) == row % layers
    acc = jnp.sum(total, axis=0, keepdims=True)
    part[...] = acc
    parts[group] = acc

    for g in range(tokens // per_tile):
        j, tile = divmod(g, row_tiles)
        c = jnp.concatenate([xv[:, g * per_tile + i, :] for i in range(per_tile)], axis=0)
        for f in range(pieces):
            centered[tile, f, j] = c[:, f * LANES:(f + 1) * LANES]

    def send_part(source, d, sem):
        pltpu.make_async_remote_copy(
            src_ref=source, dst_ref=parts.at[group], send_sem=e_send, recv_sem=sem,
            device_id=(section, d), device_id_type=MESH).start()

    def energies(count, sem):
        span = parts.at[pl.ds(0, count)]
        return pltpu.make_async_remote_copy(
            src_ref=span, dst_ref=span, send_sem=e_send, recv_sem=sem,
            device_id=(section, group), device_id_type=MESH)

    def source(u, d):
        if u < narrow:
            return centered.at[:, wide_chunks + lax.rem(d, side) * narrow + u]
        if u > narrow:
            return late[u - narrow - 1].at[:, pl.ds(d * per_dev, per_dev)]
        piece = d * each
        return centered.at[pl.ds(lax.rem(piece, row_tiles), 1), piece // row_tiles]

    def slot(u):
        return pl.ds((spot if u < narrow else group) * per_dev, per_dev)

    def spread(u, d):
        pltpu.make_async_remote_copy(
            src_ref=source(u, d), dst_ref=r1[u].at[:, slot(u)], send_sem=send1.at[u], recv_sem=recv1.at[u],
            device_id=(section, d), device_id_type=MESH).start()

    def circle(kind):
        if kind == 'near':
            return [peer_of(p) for p in sorted(range(1, groups), key=lambda p: min(p, groups - p))]
        if kind == 'rot':
            return [peer_of(p) for p in range(1, groups)]
        return [across(k) for k in range(side)] + [beside(k) for k in range(1, side)]

    pl.semaphore_wait(barrier, groups + sections - 2)
    for d in circle('near'):
        send_part(part, d, e_recv)
    if EFIRST == 1:
        for d in circle(ORDE):
            spread(narrow, d)
    elif EFIRST == 2:
        for k in range(side):
            spread(narrow, across(k))
    for u in range(narrow):
        for k in range(1, side):
            spread(u, beside(k))
        if EFIRST == 2 and u == 0:
            for k in range(1, side):
                spread(narrow, beside(k))

    load_owners.wait()

    @pl.loop(0, blocks)
    def _(o):
        found = jnp.int32(0)
        for b in range(blocks):
            found = jnp.where(owners[b] == o, jnp.int32(b), found)
        inverse[o] = found

    for u in range(narrow + 1):
        r1[u][:, slot(u)] = source(u, group)[...]
    energies(groups - 1, e_recv).wait_recv()
    total = parts[0]
    for g in range(1, groups):
        total = total + parts[g]
    energy = jnp.sum(jnp.where(own_lanes, total, 0.0), axis=1, keepdims=True)
    scale = 1.0 / jnp.sqrt(energy * (1.0 / (tokens * groups * features)) + 1.0)

    for u in range(narrow + 1, units):
        for n, i in enumerate(kinds[u - narrow]):
            for d in range(groups):
                chunk, tile = divmod(d * each + i, row_tiles)
                for j in range(per_dev):
                    late[u - narrow - 1][n, d * per_dev + j] = (centered[tile, chunk, j] * scale).astype(jnp.bfloat16)
        for d in circle(ORDL):
            spread(u, d)
        r1[u][:, slot(u)] = late[u - narrow - 1][:, slot(u)]

    def arrived(u):
        span = r1[u].at[:, pl.ds(0, ((side if u < narrow else groups) - 1) * per_dev)]
        return pltpu.make_async_remote_copy(
            src_ref=span, dst_ref=span, send_sem=send1.at[u], recv_sem=recv1.at[u],
            device_id=(section, group), device_id_type=MESH)

    def delivered(u):
        span = r2[u].at[pl.ds(0, sections * groups - 1)]
        return pltpu.make_async_remote_copy(
            src_ref=span, dst_ref=span, send_sem=send2.at[u], recv_sem=recv2.at[u],
            device_id=(section, group), device_id_type=MESH)

    plane, corner = group // quarter, lax.rem(group, quarter)

    def take(u, o):
        b = inverse[o]
        if u < narrow:
            b = lax.rem(b, side * per_dev)
        got = [r1[u][tile, b] for tile in range(r1[u].shape[0])]
        return [(v * scale).astype(jnp.bfloat16) for v in got] if u <= narrow else got

    def deliver(u, planes):
        if SPLIT:
            routes = [(t, k, q) for k in range(quarter) for q in range(sections) for t in planes]
        else:
            routes = [(t, k, q) for t in planes for k in range(quarter) for q in range(sections)]

        def place(t, k, q):
            sec, d = lax.rem(section + q, sections), t * quarter + lax.rem(corner + k, quarter)
            return sec, d, sec * groups + d

        def select(t, k, q):
            o = place(t, k, q)[2]
            for tile, block in enumerate(take(u, o)):
                s2[u][o, tile] = block

        def send(t, k, q):
            sec, d, o = place(t, k, q)

            def go():
                pltpu.make_async_remote_copy(
                    src_ref=s2[u].at[o], dst_ref=r2[u].at[me], send_sem=send2.at[u], recv_sem=recv2.at[u],
                    device_id=(sec, d), device_id_type=MESH).start()
            if k or q:
                go()
            else:
                pl.when(plane != t)(go)

        for n in range(len(routes) + LAG):
            if n < len(routes):
                select(*routes[n])
            if n >= LAG:
                send(*routes[n - LAG])

    steps = STEPS if units == NUNITS else [(u, (0, 1, 2, 3)) for u in range(units)]
    seen = []
    for u, planes in steps:
        if u not in seen:
            arrived(u).wait_recv()
            seen.append(u)
        deliver(u, planes)
    for u in seen:
        for tile, block in enumerate(take(u, me)):
            r2[u][me, tile] = block
    order = seen

    home = inverse[me] // (side * per_dev) * side

    def assemble(tile, chunk, got):
        for i in range(per_tile):
            out_ref[tile * per_tile + i, :, chunk * LANES:(chunk + 1) * LANES] = jnp.concatenate(
                [v[i * layers:(i + 1) * layers] for v in got], axis=0).astype(jnp.bfloat16)

    for u in order:
        delivered(u).wait_recv()
        if u < narrow:
            for d in range(side):
                for tile in range(row_tiles):
                    assemble(tile, wide_chunks + d * narrow + u,
                             [r2[u][s * groups + home + d, tile].astype(jnp.float32) for s in range(sections)])
        else:
            for d in range(groups):
                for n, i in enumerate(kinds[u - narrow]):
                    chunk, tile = divmod(d * each + i, row_tiles)
                    assemble(tile, chunk, [r2[u][s * groups + d, n].astype(jnp.float32) for s in range(sections)])

    energies(groups - 1, e_recv).wait_send()
    for u in range(units):
        arrived(u).wait_send()
        delivered(u).wait_send()


def store_kernel(assembled, out_hbm, sem):
    store = pltpu.make_async_copy(assembled, out_hbm, sem)
    store.start()
    store.wait()


def solution(mesh):
    sections, groups = mesh.shape["section"], mesh.shape["dp"]

    def on_device(residuals, owners):
        layers, tokens, features = residuals.shape
        blocks = owners.shape[0]
        per_dev = blocks // groups
        block_len = tokens // per_dev
        row_tiles = block_len * layers // SUBLANES
        pieces, side = features // LANES * row_tiles, groups // 2
        narrow = 1
        each = (pieces - narrow * row_tiles * side) // groups
        if LSPLIT:
            kinds = [[i] for i in range(each)]
        else:
            kinds = [[0]] + ([list(range(1, each))] if each > 1 else [])
        units = narrow + len(kinds)
        tile = (SUBLANES, LANES)
        dma = pltpu.SemaphoreType.DMA
        tiles_of = [row_tiles] * narrow + [len(k) for k in kinds]
        received = pl.pallas_call(
            functools.partial(harvest_kernel, sections, groups, narrow, kinds),
            out_shape=pltpu.VMEM((block_len, layers * sections, features), jnp.bfloat16),
            in_specs=[pl.BlockSpec(memory_space=pl.ANY), pl.BlockSpec(memory_space=pl.ANY)],
            out_specs=pl.BlockSpec(memory_space=pltpu.VMEM),
            scratch_shapes=[
                pltpu.SMEM((blocks,), jnp.int32),
                pltpu.SMEM((blocks,), jnp.int32),
                pltpu.VMEM((layers, tokens, features), jnp.float32),
                pltpu.VMEM((row_tiles, features // LANES, per_dev, *tile), jnp.float32),
                pltpu.VMEM((1, LANES), jnp.float32),
                pltpu.VMEM((groups, 1, LANES), jnp.float32),
                dma, dma, dma, dma,
                *[dma((units,)) for _ in range(4)],
                *[pltpu.VMEM((tiles_of[u], blocks // (2 if u < narrow else 1), *tile),
                             jnp.float32 if u <= narrow else jnp.bfloat16) for u in range(units)],
                *[pltpu.VMEM((blocks, tiles_of[u], *tile), jnp.bfloat16) for u in range(units)] * 2,
                *[pltpu.VMEM((len(k), blocks, *tile), jnp.bfloat16) for k in kinds[1:]],
            ],
            compiler_params=pltpu.CompilerParams(collective_id=0, has_side_effects=True),
            name="harvest",
        )(residuals, owners)
        return pl.pallas_call(
            store_kernel,
            out_shape=jax.ShapeDtypeStruct(received.shape, received.dtype),
            in_specs=[pl.BlockSpec(memory_space=pltpu.VMEM)],
            out_specs=pl.BlockSpec(memory_space=pl.ANY),
            scratch_shapes=[pltpu.SemaphoreType.DMA],
            name="store",
        )(pltpu.with_memory_space_constraint(received, pltpu.VMEM))

    in_specs = (P("section", "dp", None), P())
    out_specs = P(("section", "dp"), None, None)
    return jax.shard_map(on_device, mesh=mesh, in_specs=in_specs, out_specs=out_specs, check_vma=False)
```

```python
import functools

import jax
import jax.numpy as jnp
from jax import lax
from jax.experimental import pallas as pl
from jax.experimental.pallas import tpu as pltpu
from jax.sharding import PartitionSpec as P

MESH = pl.DeviceIdType.MESH
LANES = 128
SUBLANES = 8
LAG = 8
SHARE = 0
JOINED = 1
LI = 1
ABS = 2
STAGED = 0
LOW = (0, 1, 2)
ORDL = 'near'
ORDE = 'near'
PRE = ((1,), (0,), (2,))
STEPS = ((0, (0, 2)), (1, (0, 2, 3)), (0, ((1, 'a'), 3)), (2, (0, 2, 3)), (1, ((1, 'a'),)), (2, ((1, 'a'),)),
         (0, ((1, 'b'),)), (1, ((1, 'b'),)), (2, ((1, 'b'),)))


def layout(row_tiles, per_dev, each):
    share = per_dev // SHARE if SHARE else 0
    boxes = [(True, None, 0, per_dev, True), (False, 0, 0, per_dev, True)]
    units = [[0], [1]]
    rest = []
    for piece in range(1, each):
        cut = share if piece == 1 else 0
        if cut:
            boxes.append((False, piece, 0, cut, True))
        boxes.append((False, piece, cut, per_dev, False))
        rest.append(piece)
    units += [rest] if JOINED and rest else [[p] for p in rest]
    return boxes, units


def harvest_kernel(sections, groups, each, x_hbm, owners_hbm, out_ref, owners, inverse, xv, centered, part,
                   parts, x_sem, o_sem, e_send, e_recv, ready, send1, recv1, send2, recv2, *buffers):
    layers, tokens, features = x_hbm.shape
    pieces = features // LANES
    blocks = owners.shape[0]
    per_dev = blocks // groups
    side, quarter = groups // 2, groups // 4
    row_tiles = centered.shape[0]
    wide_chunks = groups * each // row_tiles
    boxes, units = layout(row_tiles, per_dev, each)
    nb, nu = len(boxes), len(units)
    r1, s2, r2, late = buffers[:nb], buffers[nb:nb + nu], buffers[nb + nu:nb + 2 * nu], buffers[nb + 2 * nu:]
    late = dict(zip([b for b in range(nb) if not boxes[b][4]], late))
    section, group = lax.axis_index("section"), lax.axis_index("dp")
    me = section * groups + group
    upper = group // side
    spot, base = lax.rem(group, side), upper * side

    load = pltpu.make_async_copy(x_hbm, xv, x_sem)
    load.start()
    load_owners = pltpu.make_async_copy(owners_hbm, owners, o_sem)
    load_owners.start()
    barrier = pltpu.get_barrier_semaphore()

    def peer_of(p):
        return lax.rem(group + p, groups)

    def beside(k):
        return base + lax.rem(spot + k, side)

    def across(k):
        return side - base + lax.rem(spot + k, side)

    def signal(sem, d):
        pl.semaphore_signal(sem, inc=1, device_id=(section, d), device_id_type=MESH)

    plane, corner = group // quarter, lax.rem(group, quarter)

    def member(t, k):
        return t * quarter + lax.rem(corner + k, quarter)

    for t in range(4):
        for k in range(quarter):
            if t == 0 and STAGED:
                pl.when((plane == 1) | (plane == 0) if k else plane == 1)(lambda: signal(barrier, member(t, k)))
            elif k:
                signal(barrier, member(t, k))
            else:
                pl.when(plane != t)(lambda: signal(barrier, member(t, k)))
    for k in range(1, sections):
        pl.semaphore_signal(barrier, inc=1, device_id=(lax.rem(section + k, sections), group), device_id_type=MESH)

    load.wait()
    per_tile = SUBLANES // layers
    lane = lax.broadcasted_iota(jnp.int32, (SUBLANES, LANES), 1)
    row = lax.broadcasted_iota(jnp.int32, (SUBLANES, LANES), 0)
    total = jnp.zeros((SUBLANES, LANES), jnp.float32)
    for l in range(layers):
        acc = jnp.zeros((SUBLANES, LANES), jnp.float32)
        for t in range(0, tokens, SUBLANES):
            x = xv[l, t:t + SUBLANES]
            c = x - jnp.sum(x, axis=1, keepdims=True) * (1.0 / features)
            xv[l, t:t + SUBLANES] = c
            sq = c * c
            for f in range(pieces):
                acc = acc + sq[:, f * LANES:(f + 1) * LANES]
        fold = LANES // 2
        while fold >= LANES // layers:
            acc = acc + pltpu.roll(acc, fold, 1)
            fold //= 2
        total = total + jnp.where(lane // (LANES // layers) == l, acc, 0.0)
    own_lanes = lane // (LANES // layers) == row % layers
    acc = jnp.sum(total, axis=0, keepdims=True)
    part[...] = acc
    parts[group] = acc

    for g in range(tokens // per_tile):
        j, tile = divmod(g, row_tiles)
        c = jnp.concatenate([xv[:, g * per_tile + i, :] for i in range(per_tile)], axis=0)
        for f in range(pieces):
            centered[tile, f, j] = c[:, f * LANES:(f + 1) * LANES]

    def send_part(source, d, sem):
        pltpu.make_async_remote_copy(
            src_ref=source, dst_ref=parts.at[group], send_sem=e_send, recv_sem=sem,
            device_id=(section, d), device_id_type=MESH).start()

    def energies(count, sem):
        span = parts.at[pl.ds(0, count)]
        return pltpu.make_async_remote_copy(
            src_ref=span, dst_ref=span, send_sem=e_send, recv_sem=sem,
            device_id=(section, group), device_id_type=MESH)

    def source(b, d):
        half, piece, low, high, raw = boxes[b]
        if half:
            return centered.at[:, wide_chunks + lax.rem(d, side)]
        if not raw:
            return late[b].at[:, pl.ds(d * (high - low), high - low)]
        at = d * each + piece
        return centered.at[pl.ds(lax.rem(at, row_tiles), 1), at // row_tiles, pl.ds(low, high - low)]

    def slot(b):
        half, _, low, high, _ = boxes[b]
        return pl.ds((spot if half else group) * (high - low), high - low)

    def spread(*group_of, peers=None):
        first = group_of[0]
        if peers is None:
            peers = [beside(k) for k in range(1, side)] if boxes[first][0] else circle(ORDE if boxes[first][4] else ORDL)
        for d, b in [(d, b) for d in peers for b in group_of]:
            pltpu.make_async_remote_copy(
                src_ref=source(b, d), dst_ref=r1[b].at[:, slot(b)], send_sem=send1.at[b], recv_sem=recv1.at[b],
                device_id=(section, d), device_id_type=MESH).start()

    def circle(kind):
        if kind == 'near':
            return [peer_of(p) for p in sorted(range(1, groups), key=lambda p: min(p, groups - p))]
        if kind == 'rot':
            return [peer_of(p) for p in range(1, groups)]
        return [across(k) for k in range(side)] + [beside(k) for k in range(1, side)]

    early = [b for b in range(nb) if boxes[b][4]]

    def full_start():
        for d in circle('near'):
            send_part(part, d, e_recv)
        for bs in PRE:
            bs = [b for b in bs if b in early]
            if bs:
                spread(*bs)

    if STAGED:
        some = (plane + 3) // 4
        pl.semaphore_wait(barrier, side - 1 + sections - 1 + side * some)

        @pl.when(plane == 0)
        def _():
            nearby = [beside(k) for k in range(1, side)]
            distant = [across(k) for k in range(side)]
            for d in nearby:
                send_part(part, d, e_recv)
            for b in LOW:
                if b in early:
                    spread(b, peers=nearby)
            pl.semaphore_wait(ready, 1)
            for d in distant:
                send_part(part, d, e_recv)
            for b in LOW:
                if b in early and b:
                    spread(b, peers=distant)

        @pl.when(plane >= 1)
        def _():
            pl.when(plane == 1)(lambda: signal(ready, group - quarter))
            full_start()
    else:
        pl.semaphore_wait(barrier, groups + sections - 2)
        full_start()

    load_owners.wait()

    @pl.loop(0, blocks)
    def _(o):
        found = jnp.int32(0)
        for b in range(blocks):
            found = jnp.where(owners[b] == o, jnp.int32(b), found)
        inverse[o] = found

    for b in early:
        r1[b][:, slot(b)] = source(b, group)[...]
    energies(groups - 1, e_recv).wait_recv()
    total = parts[0]
    for g in range(1, groups):
        total = total + parts[g]
    energy = jnp.sum(jnp.where(own_lanes, total, 0.0), axis=1, keepdims=True)
    scale = 1.0 / jnp.sqrt(energy * (1.0 / (tokens * groups * features)) + 1.0)

    for b, out in late.items():
        _, piece, low, high, _ = boxes[b]
        for d in range(groups):
            chunk, tile = divmod(d * each + piece, row_tiles)
            for j in range(low, high):
                out[0, d * (high - low) + j - low] = (centered[tile, chunk, j] * scale).astype(jnp.bfloat16)
        if not LI:
            spread(b)
    if late and LI:
        spread(*late)
    for b, out in late.items():
        r1[b][:, slot(b)] = out[:, slot(b)]

    def arrived(b):
        half, _, low, high, _ = boxes[b]
        span = r1[b].at[:, pl.ds(0, ((side if half else groups) - 1) * (high - low))]
        return pltpu.make_async_remote_copy(
            src_ref=span, dst_ref=span, send_sem=send1.at[b], recv_sem=recv1.at[b],
            device_id=(section, group), device_id_type=MESH)

    def delivered(u):
        span = r2[u].at[pl.ds(0, sections * groups - 1)]
        return pltpu.make_async_remote_copy(
            src_ref=span, dst_ref=span, send_sem=send2.at[u], recv_sem=recv2.at[u],
            device_id=(section, group), device_id_type=MESH)

    def boxes_of(piece):
        return [b for b in range(nb) if boxes[b][1] == piece and not boxes[b][0]]

    def needs(u):
        return [0] if u == 0 else [b for piece in (units[u] if u > 1 else [0]) for b in boxes_of(piece)]

    def scaled(v):
        return (v * scale).astype(jnp.bfloat16)

    def take(u, o):
        at = inverse[o]
        if u == 0:
            at = lax.rem(at, side * per_dev)
            return [scaled(r1[0][tile, at]) for tile in range(row_tiles)]
        if u == 1:
            return [scaled(r1[1][0, at])]
        got = []
        for piece in units[u]:
            which = boxes_of(piece)
            if len(which) == 1:
                got.append(r1[which[0]][0, at])
            else:
                cut = boxes[which[0]][3]
                d, j = at // per_dev, lax.rem(at, per_dev)
                first = scaled(r1[which[0]][0, d * cut + lax.rem(j, cut)])
                second = r1[which[1]][0, d * (per_dev - cut) + lax.rem(j, per_dev - cut)]
                got.append(jnp.where(j < cut, first, second))
        return got

    def deliver(u, planes):
        if ABS == 1:
            keys = [(h, c, q) for q in range(sections) for h in range(quarter // 2) for c in range(2)]
        elif ABS == 2:
            keys = [(h, c, q) for h in range(quarter // 2) for q in range(sections) for c in range(2)]
        elif ABS == 3:
            keys = [(h, c, q) for h in range(quarter // 2) for c in range(2) for q in range(sections)]
        else:
            keys = [(h, c, q) for h in range(quarter // 2) for c in range(2) for q in range(sections)]
        routes = []
        for t in planes:
            t, part = t if isinstance(t, tuple) else (t, None)
            routes += [(t, k, k[2]) for k in keys if part is None or (part == 'a') == (k[0] == 0 and k[2] == 0)]

        def place(t, k, q):
            h, c, _ = k
            if ABS:
                sec, d = jnp.int32(q), t * quarter + h * 2 + lax.rem(corner + c, 2)
            else:
                sec, d = lax.rem(section + q, sections), t * quarter + lax.rem(corner + h * 2 + c, quarter)
            return sec, d, sec * groups + d

        def select(t, k, q):
            o = place(t, k, q)[2]
            for tile, block in enumerate(take(u, o)):
                s2[u][o, tile] = block

        def send(t, k, q):
            sec, d, o = place(t, k, q)

            def go():
                pltpu.make_async_remote_copy(
                    src_ref=s2[u].at[o], dst_ref=r2[u].at[me], send_sem=send2.at[u], recv_sem=recv2.at[u],
                    device_id=(sec, d), device_id_type=MESH).start()
            h, c, _ = k
            if ABS and not c:
                pl.when((plane != t) | (section != q) | (corner // 2 != h))(go)
            elif not ABS and not (h or c or q):
                pl.when(plane != t)(go)
            else:
                go()

        for n in range(len(routes) + LAG):
            if n < len(routes):
                select(*routes[n])
            if n >= LAG:
                send(*routes[n - LAG])

    steps = STEPS if nu == max(u for u, _ in STEPS) + 1 else [(u, (0, 1, 2, 3)) for u in range(nu)]
    seen = []
    for u, planes in steps:
        if u not in seen:
            for b in needs(u):
                arrived(b).wait_recv()
            seen.append(u)
        deliver(u, planes)
    for u in seen:
        for tile, block in enumerate(take(u, me)):
            r2[u][me, tile] = block
    order = seen

    home = inverse[me] // (side * per_dev) * side

    def assemble(tile, chunk, got):
        for i in range(per_tile):
            out_ref[tile * per_tile + i, :, chunk * LANES:(chunk + 1) * LANES] = jnp.concatenate(
                [v[i * layers:(i + 1) * layers] for v in got], axis=0).astype(jnp.bfloat16)

    for u in order:
        delivered(u).wait_recv()
        if u == 0:
            for d in range(side):
                for tile in range(row_tiles):
                    assemble(tile, wide_chunks + d,
                             [r2[u][s * groups + home + d, tile].astype(jnp.float32) for s in range(sections)])
        else:
            for d in range(groups):
                for n, piece in enumerate(units[u] if u > 1 else [0]):
                    chunk, tile = divmod(d * each + piece, row_tiles)
                    assemble(tile, chunk, [r2[u][s * groups + d, n].astype(jnp.float32) for s in range(sections)])

    energies(groups - 1, e_recv).wait_send()
    for b in range(nb):
        arrived(b).wait_send()
    for u in range(nu):
        delivered(u).wait_send()


def store_kernel(assembled, out_hbm, sem):
    store = pltpu.make_async_copy(assembled, out_hbm, sem)
    store.start()
    store.wait()


def solution(mesh):
    sections, groups = mesh.shape["section"], mesh.shape["dp"]

    def on_device(residuals, owners):
        layers, tokens, features = residuals.shape
        blocks = owners.shape[0]
        per_dev = blocks // groups
        block_len = tokens // per_dev
        row_tiles = block_len * layers // SUBLANES
        pieces, side = features // LANES * row_tiles, groups // 2
        each = (pieces - row_tiles * side) // groups
        boxes, units = layout(row_tiles, per_dev, each)
        tile = (SUBLANES, LANES)
        dma = pltpu.SemaphoreType.DMA
        inboxes = [(row_tiles if half else 1, (side if half else groups) * (high - low), *tile)
                   for half, _, low, high, _ in boxes]
        outboxes = [(blocks, row_tiles if u == 0 else 1 if u == 1 else len(units[u]), *tile) for u in range(len(units))]
        received = pl.pallas_call(
            functools.partial(harvest_kernel, sections, groups, each),
            out_shape=pltpu.VMEM((block_len, layers * sections, features), jnp.bfloat16),
            in_specs=[pl.BlockSpec(memory_space=pl.ANY), pl.BlockSpec(memory_space=pl.ANY)],
            out_specs=pl.BlockSpec(memory_space=pltpu.VMEM),
            scratch_shapes=[
                pltpu.SMEM((blocks,), jnp.int32),
                pltpu.SMEM((blocks,), jnp.int32),
                pltpu.VMEM((layers, tokens, features), jnp.float32),
                pltpu.VMEM((row_tiles, features // LANES, per_dev, *tile), jnp.float32),
                pltpu.VMEM((1, LANES), jnp.float32),
                pltpu.VMEM((groups, 1, LANES), jnp.float32),
                dma, dma, dma, dma, pltpu.SemaphoreType.REGULAR,
                *[dma((len(boxes),)) for _ in range(2)],
                *[dma((len(units),)) for _ in range(2)],
                *[pltpu.VMEM(inboxes[b], jnp.float32 if boxes[b][4] else jnp.bfloat16) for b in range(len(boxes))],
                *[pltpu.VMEM(shape, jnp.bfloat16) for shape in outboxes * 2],
                *[pltpu.VMEM(inboxes[b], jnp.bfloat16) for b in range(len(boxes)) if not boxes[b][4]],
            ],
            compiler_params=pltpu.CompilerParams(collective_id=0, has_side_effects=True),
            name="harvest",
        )(residuals, owners)
        return pl.pallas_call(
            store_kernel,
            out_shape=jax.ShapeDtypeStruct(received.shape, received.dtype),
            in_specs=[pl.BlockSpec(memory_space=pltpu.VMEM)],
            out_specs=pl.BlockSpec(memory_space=pl.ANY),
            scratch_shapes=[pltpu.SemaphoreType.DMA],
            name="store",
        )(pltpu.with_memory_space_constraint(received, pltpu.VMEM))

    in_specs = (P("section", "dp", None), P())
    out_specs = P(("section", "dp"), None, None)
    return jax.shard_map(on_device, mesh=mesh, in_specs=in_specs, out_specs=out_specs, check_vma=False)
```

```python
import functools

import jax
import jax.numpy as jnp
from jax import lax
from jax.experimental import pallas as pl
from jax.experimental.pallas import tpu as pltpu
from jax.sharding import PartitionSpec as P

MESH = pl.DeviceIdType.MESH
LANES = 128
SUBLANES = 8
LAG = 8
SHARE = 2
ABS = 2
ORDL = 'near'
ORDE = 'near'
PRE = ((1, 'a'), (0, 'b'), (1, 'b'), (2, 'a'), (2, 'b'))
ORDN = 'near'
STEPS = ((0, (0, 2)), (1, (0, 2, 3)), (0, ((1, 'a'), 3)), (1, ((1, 'a'),)), (2, (0, 2, 3)), (2, ((1, 'a'),)), (0, ((1, 'b'),)), (1, ((1, 'b'),)), (2, ((1, 'b'),)))


def layout(row_tiles, per_dev, each):
    share = per_dev // SHARE if SHARE else 0
    boxes = [(True, None, 0, per_dev, True, None), (False, 0, 0, per_dev, True, None)]
    for piece in range(1, each):
        cut = share if piece == 1 else 0
        if cut:
            boxes.append((False, piece, 0, cut, True, 1))
            boxes.append((False, piece, cut, per_dev, False, 1))
            boxes.append((False, piece, 0, per_dev, False, 0))
        else:
            boxes.append((False, piece, 0, per_dev, False, None))
    units = [[0], [1]] + ([list(range(1, each))] if each > 1 else [])
    return boxes, units


def harvest_kernel(sections, groups, each, x_hbm, owners_hbm, out_ref, owners, inverse, xv, centered, part,
                   parts, x_sem, o_sem, e_send, e_recv, send1, recv1, send2, recv2, *buffers):
    layers, tokens, features = x_hbm.shape
    pieces = features // LANES
    blocks = owners.shape[0]
    per_dev = blocks // groups
    side, quarter = groups // 2, groups // 4
    row_tiles = centered.shape[0]
    wide_chunks = groups * each // row_tiles
    boxes, units = layout(row_tiles, per_dev, each)
    nb, nu = len(boxes), len(units)
    r1, s2, r2, late = buffers[:nb], buffers[nb:nb + nu], buffers[nb + nu:nb + 2 * nu], buffers[nb + 2 * nu:]
    late = dict(zip([b for b in range(nb) if not boxes[b][4]], late))
    section, group = lax.axis_index("section"), lax.axis_index("dp")
    me = section * groups + group
    upper = group // side
    spot, base = lax.rem(group, side), upper * side

    load = pltpu.make_async_copy(x_hbm, xv, x_sem)
    load.start()
    load_owners = pltpu.make_async_copy(owners_hbm, owners, o_sem)
    load_owners.start()
    barrier = pltpu.get_barrier_semaphore()

    def peer_of(p):
        return lax.rem(group + p, groups)

    def beside(k):
        return base + lax.rem(spot + k, side)

    def across(k):
        return side - base + lax.rem(spot + k, side)

    def signal(sem, d):
        pl.semaphore_signal(sem, inc=1, device_id=(section, d), device_id_type=MESH)

    plane, corner = group // quarter, lax.rem(group, quarter)

    def member(t, k):
        return t * quarter + lax.rem(corner + k, quarter)

    for t in range(4):
        for k in range(quarter):
            if k:
                signal(barrier, member(t, k))
            else:
                pl.when(plane != t)(lambda: signal(barrier, member(t, k)))
    for k in range(1, sections):
        pl.semaphore_signal(barrier, inc=1, device_id=(lax.rem(section + k, sections), group), device_id_type=MESH)

    load.wait()
    per_tile = SUBLANES // layers
    lane = lax.broadcasted_iota(jnp.int32, (SUBLANES, LANES), 1)
    row = lax.broadcasted_iota(jnp.int32, (SUBLANES, LANES), 0)
    total = jnp.zeros((SUBLANES, LANES), jnp.float32)
    for l in range(layers):
        acc = jnp.zeros((SUBLANES, LANES), jnp.float32)
        for t in range(0, tokens, SUBLANES):
            x = xv[l, t:t + SUBLANES]
            c = x - jnp.sum(x, axis=1, keepdims=True) * (1.0 / features)
            xv[l, t:t + SUBLANES] = c
            sq = c * c
            for f in range(pieces):
                acc = acc + sq[:, f * LANES:(f + 1) * LANES]
        fold = LANES // 2
        while fold >= LANES // layers:
            acc = acc + pltpu.roll(acc, fold, 1)
            fold //= 2
        total = total + jnp.where(lane // (LANES // layers) == l, acc, 0.0)
    own_lanes = lane // (LANES // layers) == row % layers
    acc = jnp.sum(total, axis=0, keepdims=True)
    part[...] = acc
    parts[group] = acc

    for g in range(tokens // per_tile):
        j, tile = divmod(g, row_tiles)
        c = jnp.concatenate([xv[:, g * per_tile + i, :] for i in range(per_tile)], axis=0)
        for f in range(pieces):
            centered[tile, f, j] = c[:, f * LANES:(f + 1) * LANES]

    def send_part(source, d, sem):
        pltpu.make_async_remote_copy(
            src_ref=source, dst_ref=parts.at[group], send_sem=e_send, recv_sem=sem,
            device_id=(section, d), device_id_type=MESH).start()

    def energies(count, sem):
        span = parts.at[pl.ds(0, count)]
        return pltpu.make_async_remote_copy(
            src_ref=span, dst_ref=span, send_sem=e_send, recv_sem=sem,
            device_id=(section, group), device_id_type=MESH)

    def source(b, d):
        half, piece, low, high, raw, _ = boxes[b]
        if half:
            return centered.at[:, wide_chunks + lax.rem(d, side)]
        if not raw:
            return late[b].at[:, pl.ds(d * (high - low), high - low)]
        at = d * each + piece
        return centered.at[pl.ds(lax.rem(at, row_tiles), 1), at // row_tiles, pl.ds(low, high - low)]

    def slot(b):
        half, _, low, high, _, who = boxes[b]
        return pl.ds((spot if half or who is not None else group) * (high - low), high - low)

    def from_us(b, body):
        who = boxes[b][5]
        if who is None:
            body()
        else:
            pl.when(upper == who)(body)

    def post(b, d):
        pltpu.make_async_remote_copy(
            src_ref=source(b, d), dst_ref=r1[b].at[:, slot(b)], send_sem=send1.at[b], recv_sem=recv1.at[b],
            device_id=(section, d), device_id_type=MESH).start()

    def keep(b):
        def body():
            r1[b][:, slot(b)] = source(b, group)[...]
        from_us(b, body)

    def circle(kind):
        if kind == 'near':
            return [peer_of(p) for p in sorted(range(1, groups), key=lambda p: min(p, groups - p))]
        if kind == 'rot':
            return [peer_of(p) for p in range(1, groups)]
        return [across(k) for k in range(side)] + [beside(k) for k in range(1, side)]

    early = [b for b in range(nb) if boxes[b][4]]

    def full_start():
        for d in circle(ORDN):
            send_part(part, d, e_recv)
        for b, where in PRE:
            if b not in early:
                continue
            peers = {'a': [across(k) for k in range(side)], 'b': [beside(k) for k in range(1, side)]}.get(where)

            def body():
                for d in peers or circle(ORDE):
                    post(b, d)
            from_us(b, body)

    pl.semaphore_wait(barrier, groups + sections - 2)
    full_start()

    load_owners.wait()

    @pl.loop(0, blocks)
    def _(o):
        found = jnp.int32(0)
        for b in range(blocks):
            found = jnp.where(owners[b] == o, jnp.int32(b), found)
        inverse[o] = found

    for b in early:
        keep(b)
    energies(groups - 1, e_recv).wait_recv()
    total = parts[0]
    for g in range(1, groups):
        total = total + parts[g]
    energy = jnp.sum(jnp.where(own_lanes, total, 0.0), axis=1, keepdims=True)
    scale = 1.0 / jnp.sqrt(energy * (1.0 / (tokens * groups * features)) + 1.0)

    def fill(b):
        _, piece, low, high, _, _ = boxes[b]
        for d in range(groups):
            chunk, tile = divmod(d * each + piece, row_tiles)
            for j in range(low, high):
                late[b][0, d * (high - low) + j - low] = (centered[tile, chunk, j] * scale).astype(jnp.bfloat16)

    def finish(who):
        ours = [b for b in late if boxes[b][5] in (None, who)]
        for b in ours:
            fill(b)
        for d in circle(ORDL):
            for b in ours:
                post(b, d)

    if any(boxes[b][5] is not None for b in late):
        for who in range(2):
            pl.when(upper == who)(functools.partial(finish, who))
    elif late:
        finish(None)
    for b in late:
        keep(b)

    def span_of(b, count):
        wanted, raw = count * (boxes[b][3] - boxes[b][2]), boxes[b][4]
        model = b if wanted <= r1[b].shape[1] else next(
            m for m in range(nb) if boxes[m][4] == raw and r1[m].shape[0] == 1 and r1[m].shape[1] >= wanted)
        return r1[model].at[:, pl.ds(0, wanted)]

    def arrival(b, count):
        span = span_of(b, count)
        return pltpu.make_async_remote_copy(
            src_ref=span, dst_ref=span, send_sem=send1.at[b], recv_sem=recv1.at[b],
            device_id=(section, group), device_id_type=MESH)

    def await_box(b):
        half, _, _, _, _, who = boxes[b]
        if who is None:
            arrival(b, (side if half else groups) - 1).wait_recv()
        else:
            pl.when(upper == who)(lambda: arrival(b, side - 1).wait_recv())
            pl.when(upper != who)(lambda: arrival(b, side).wait_recv())

    def await_sent(b):
        from_us(b, lambda: arrival(b, (side if boxes[b][0] else groups) - 1).wait_send())

    def delivered(u):
        span = r2[u].at[pl.ds(0, sections * groups - 1)]
        return pltpu.make_async_remote_copy(
            src_ref=span, dst_ref=span, send_sem=send2.at[u], recv_sem=recv2.at[u],
            device_id=(section, group), device_id_type=MESH)

    def boxes_of(piece):
        return [b for b in range(nb) if boxes[b][1] == piece and not boxes[b][0]]

    def needs(u):
        return [0] if u == 0 else [b for piece in (units[u] if u > 1 else [0]) for b in boxes_of(piece)]

    def scaled(v):
        return (v * scale).astype(jnp.bfloat16)

    def take(u, o):
        at = inverse[o]
        if u == 0:
            at = lax.rem(at, side * per_dev)
            return [scaled(r1[0][tile, at]) for tile in range(row_tiles)]
        if u == 1:
            return [scaled(r1[1][0, at])]
        got = []
        for piece in units[u]:
            which = boxes_of(piece)
            if len(which) == 1:
                got.append(r1[which[0]][0, at])
            else:
                cut = boxes[which[0]][3]
                d, j = at // per_dev, lax.rem(at, per_dev)
                place = lax.rem(d, side)
                first = scaled(r1[which[0]][0, place * cut + lax.rem(j, cut)])
                second = r1[which[1]][0, place * (per_dev - cut) + lax.rem(j, per_dev - cut)]
                third = r1[which[2]][0, place * per_dev + j]
                got.append(jnp.where(d < side, third, jnp.where(j < cut, first, second)))
        return got

    def deliver(u, planes):
        if ABS == 1:
            keys = [(h, c, q) for q in range(sections) for h in range(quarter // 2) for c in range(2)]
        elif ABS == 2:
            keys = [(h, c, q) for h in range(quarter // 2) for q in range(sections) for c in range(2)]
        elif ABS == 3:
            keys = [(h, c, q) for h in range(quarter // 2) for c in range(2) for q in range(sections)]
        else:
            keys = [(h, c, q) for h in range(quarter // 2) for c in range(2) for q in range(sections)]
        routes = []
        for t in planes:
            t, part = t if isinstance(t, tuple) else (t, None)
            routes += [(t, k, k[2]) for k in keys if part is None or (part == 'a') == (k[0] == 0 and k[2] == 0)]

        def place(t, k, q):
            h, c, _ = k
            if ABS:
                sec, d = jnp.int32(q), t * quarter + h * 2 + lax.rem(corner + c, 2)
            else:
                sec, d = lax.rem(section + q, sections), t * quarter + lax.rem(corner + h * 2 + c, quarter)
            return sec, d, sec * groups + d

        def select(t, k, q):
            o = place(t, k, q)[2]
            for tile, block in enumerate(take(u, o)):
                s2[u][o, tile] = block

        def send(t, k, q):
            sec, d, o = place(t, k, q)

            def go():
                pltpu.make_async_remote_copy(
                    src_ref=s2[u].at[o], dst_ref=r2[u].at[me], send_sem=send2.at[u], recv_sem=recv2.at[u],
                    device_id=(sec, d), device_id_type=MESH).start()
            h, c, _ = k
            if ABS and not c:
                pl.when((plane != t) | (section != q) | (corner // 2 != h))(go)
            elif not ABS and not (h or c or q):
                pl.when(plane != t)(go)
            else:
                go()

        for n in range(len(routes) + LAG):
            if n < len(routes):
                select(*routes[n])
            if n >= LAG:
                send(*routes[n - LAG])

    steps = STEPS if nu == max(u for u, _ in STEPS) + 1 else [(u, (0, 1, 2, 3)) for u in range(nu)]
    seen = []
    for u, planes in steps:
        if u not in seen:
            for b in needs(u):
                await_box(b)
            seen.append(u)
        deliver(u, planes)
    for u in seen:
        for tile, block in enumerate(take(u, me)):
            r2[u][me, tile] = block
    order = seen

    home = inverse[me] // (side * per_dev) * side

    def assemble(tile, chunk, got):
        for i in range(per_tile):
            out_ref[tile * per_tile + i, :, chunk * LANES:(chunk + 1) * LANES] = jnp.concatenate(
                [v[i * layers:(i + 1) * layers] for v in got], axis=0).astype(jnp.bfloat16)

    for u in order:
        delivered(u).wait_recv()
        if u == 0:
            for d in range(side):
                for tile in range(row_tiles):
                    assemble(tile, wide_chunks + d,
                             [r2[u][s * groups + home + d, tile].astype(jnp.float32) for s in range(sections)])
        else:
            for d in range(groups):
                for n, piece in enumerate(units[u] if u > 1 else [0]):
                    chunk, tile = divmod(d * each + piece, row_tiles)
                    assemble(tile, chunk, [r2[u][s * groups + d, n].astype(jnp.float32) for s in range(sections)])

    energies(groups - 1, e_recv).wait_send()
    for b in range(nb):
        await_sent(b)
    for u in range(nu):
        delivered(u).wait_send()


def store_kernel(assembled, out_hbm, sem):
    store = pltpu.make_async_copy(assembled, out_hbm, sem)
    store.start()
    store.wait()


def solution(mesh):
    sections, groups = mesh.shape["section"], mesh.shape["dp"]

    def on_device(residuals, owners):
        layers, tokens, features = residuals.shape
        blocks = owners.shape[0]
        per_dev = blocks // groups
        block_len = tokens // per_dev
        row_tiles = block_len * layers // SUBLANES
        pieces, side = features // LANES * row_tiles, groups // 2
        each = (pieces - row_tiles * side) // groups
        boxes, units = layout(row_tiles, per_dev, each)
        tile = (SUBLANES, LANES)
        dma = pltpu.SemaphoreType.DMA
        inboxes = [(row_tiles if half else 1, (side if half or who is not None else groups) * (high - low), *tile)
                   for half, _, low, high, _, who in boxes]
        outboxes = [(blocks, row_tiles if u == 0 else 1 if u == 1 else len(units[u]), *tile) for u in range(len(units))]
        received = pl.pallas_call(
            functools.partial(harvest_kernel, sections, groups, each),
            out_shape=pltpu.VMEM((block_len, layers * sections, features), jnp.bfloat16),
            in_specs=[pl.BlockSpec(memory_space=pl.ANY), pl.BlockSpec(memory_space=pl.ANY)],
            out_specs=pl.BlockSpec(memory_space=pltpu.VMEM),
            scratch_shapes=[
                pltpu.SMEM((blocks,), jnp.int32),
                pltpu.SMEM((blocks,), jnp.int32),
                pltpu.VMEM((layers, tokens, features), jnp.float32),
                pltpu.VMEM((row_tiles, features // LANES, per_dev, *tile), jnp.float32),
                pltpu.VMEM((1, LANES), jnp.float32),
                pltpu.VMEM((groups, 1, LANES), jnp.float32),
                dma, dma, dma, dma,
                *[dma((len(boxes),)) for _ in range(2)],
                *[dma((len(units),)) for _ in range(2)],
                *[pltpu.VMEM(inboxes[b], jnp.float32 if boxes[b][4] else jnp.bfloat16) for b in range(len(boxes))],
                *[pltpu.VMEM(shape, jnp.bfloat16) for shape in outboxes * 2],
                *[pltpu.VMEM((1, groups * (b[3] - b[2]), *tile), jnp.bfloat16) for b in boxes if not b[4]],
            ],
            compiler_params=pltpu.CompilerParams(collective_id=0, has_side_effects=True),
            name="harvest",
        )(residuals, owners)
        return pl.pallas_call(
            store_kernel,
            out_shape=jax.ShapeDtypeStruct(received.shape, received.dtype),
            in_specs=[pl.BlockSpec(memory_space=pltpu.VMEM)],
            out_specs=pl.BlockSpec(memory_space=pl.ANY),
            scratch_shapes=[pltpu.SemaphoreType.DMA],
            name="store",
        )(pltpu.with_memory_space_constraint(received, pltpu.VMEM))

    in_specs = (P("section", "dp", None), P())
    out_specs = P(("section", "dp"), None, None)
    return jax.shard_map(on_device, mesh=mesh, in_specs=in_specs, out_specs=out_specs, check_vma=False)
```

```python
import functools

import jax
import jax.numpy as jnp
from jax import lax
from jax.experimental import pallas as pl
from jax.experimental.pallas import tpu as pltpu
from jax.sharding import PartitionSpec as P

MESH = pl.DeviceIdType.MESH
LANES = 128
SUBLANES = 8
LAG = 8
SHARE = 2
WHO = 1
PRE = ((1, 'a'), (0, 'b'), (1, 'b'), (2, 'a'), (2, 'b'))
STEPS = ((0, (0, 2)), (1, (0, 2, 3)), (0, ((1, 'a'), 3)), (1, ((1, 'a'),)), (2, (0, 2, 3)), (2, ((1, 'a'),)), (0, ((1, 'b'),)), (1, ((1, 'b'),)), (2, ((1, 'b'),)))


def layout(row_tiles, per_dev, each):
    share = per_dev // SHARE
    boxes = [(True, None, 0, per_dev, True, None), (False, 0, 0, per_dev, True, None)]
    for piece in range(1, each):
        cut = share if piece == 1 else 0
        if cut:
            boxes.append((False, piece, 0, cut, True, WHO))
            boxes.append((False, piece, cut, per_dev, False, WHO))
            boxes.append((False, piece, 0, per_dev, False, 1 - WHO))
        else:
            boxes.append((False, piece, 0, per_dev, False, None))
    units = [[0], [1]] + ([list(range(1, each))] if each > 1 else [])
    return boxes, units


def harvest_kernel(sections, groups, each, x_hbm, owners_hbm, out_ref, owners, inverse, xv, centered, part,
                   parts, x_sem, o_sem, e_send, e_recv, send1, recv1, send2, recv2, *buffers):
    layers, tokens, features = x_hbm.shape
    pieces = features // LANES
    blocks = owners.shape[0]
    per_dev = blocks // groups
    side, quarter = groups // 2, groups // 4
    row_tiles = centered.shape[0]
    wide_chunks = groups * each // row_tiles
    boxes, units = layout(row_tiles, per_dev, each)
    nb, nu = len(boxes), len(units)
    r1, s2, r2, late = buffers[:nb], buffers[nb:nb + nu], buffers[nb + nu:nb + 2 * nu], buffers[nb + 2 * nu:]
    late = dict(zip([b for b in range(nb) if not boxes[b][4]], late))
    section, group = lax.axis_index("section"), lax.axis_index("dp")
    me = section * groups + group
    upper = group // side
    spot, base = lax.rem(group, side), upper * side

    load = pltpu.make_async_copy(x_hbm, xv, x_sem)
    load.start()
    load_owners = pltpu.make_async_copy(owners_hbm, owners, o_sem)
    load_owners.start()
    barrier = pltpu.get_barrier_semaphore()

    def peer_of(p):
        return lax.rem(group + p, groups)

    def beside(k):
        return base + lax.rem(spot + k, side)

    def across(k):
        return side - base + lax.rem(spot + k, side)

    def signal(sem, d):
        pl.semaphore_signal(sem, inc=1, device_id=(section, d), device_id_type=MESH)

    plane, corner = group // quarter, lax.rem(group, quarter)

    def member(t, k):
        return t * quarter + lax.rem(corner + k, quarter)

    for t in range(4):
        for k in range(quarter):
            if k:
                signal(barrier, member(t, k))
            else:
                pl.when(plane != t)(lambda: signal(barrier, member(t, k)))
    for k in range(1, sections):
        pl.semaphore_signal(barrier, inc=1, device_id=(lax.rem(section + k, sections), group), device_id_type=MESH)

    load.wait()
    per_tile = SUBLANES // layers
    lane = lax.broadcasted_iota(jnp.int32, (SUBLANES, LANES), 1)
    row = lax.broadcasted_iota(jnp.int32, (SUBLANES, LANES), 0)
    total = jnp.zeros((SUBLANES, LANES), jnp.float32)
    for l in range(layers):
        acc = jnp.zeros((SUBLANES, LANES), jnp.float32)
        for t in range(0, tokens, SUBLANES):
            x = xv[l, t:t + SUBLANES]
            c = x - jnp.sum(x, axis=1, keepdims=True) * (1.0 / features)
            xv[l, t:t + SUBLANES] = c
            sq = c * c
            for f in range(pieces):
                acc = acc + sq[:, f * LANES:(f + 1) * LANES]
        fold = LANES // 2
        while fold >= LANES // layers:
            acc = acc + pltpu.roll(acc, fold, 1)
            fold //= 2
        total = total + jnp.where(lane // (LANES // layers) == l, acc, 0.0)
    own_lanes = lane // (LANES // layers) == row % layers
    acc = jnp.sum(total, axis=0, keepdims=True)
    part[...] = acc
    parts[group] = acc

    for g in range(tokens // per_tile):
        j, tile = divmod(g, row_tiles)
        c = jnp.concatenate([xv[:, g * per_tile + i, :] for i in range(per_tile)], axis=0)
        for f in range(pieces):
            centered[tile, f, j] = c[:, f * LANES:(f + 1) * LANES]

    def send_part(source, d, sem):
        pltpu.make_async_remote_copy(
            src_ref=source, dst_ref=parts.at[group], send_sem=e_send, recv_sem=sem,
            device_id=(section, d), device_id_type=MESH).start()

    def energies(count, sem):
        span = parts.at[pl.ds(0, count)]
        return pltpu.make_async_remote_copy(
            src_ref=span, dst_ref=span, send_sem=e_send, recv_sem=sem,
            device_id=(section, group), device_id_type=MESH)

    def source(b, d):
        half, piece, low, high, raw, _ = boxes[b]
        if half:
            return centered.at[:, wide_chunks + lax.rem(d, side)]
        if not raw:
            return late[b].at[:, pl.ds(d * (high - low), high - low)]
        at = d * each + piece
        return centered.at[pl.ds(lax.rem(at, row_tiles), 1), at // row_tiles, pl.ds(low, high - low)]

    def slot(b):
        half, _, low, high, _, who = boxes[b]
        return pl.ds((spot if half or who is not None else group) * (high - low), high - low)

    def from_us(b, body):
        who = boxes[b][5]
        if who is None:
            body()
        else:
            pl.when(upper == who)(body)

    def post(b, d):
        pltpu.make_async_remote_copy(
            src_ref=source(b, d), dst_ref=r1[b].at[:, slot(b)], send_sem=send1.at[b], recv_sem=recv1.at[b],
            device_id=(section, d), device_id_type=MESH).start()

    def keep(b):
        def body():
            r1[b][:, slot(b)] = source(b, group)[...]
        from_us(b, body)

    around = [peer_of(p) for p in sorted(range(1, groups), key=lambda p: min(p, groups - p))]

    early = [b for b in range(nb) if boxes[b][4]]

    pl.semaphore_wait(barrier, groups + sections - 2)
    for d in around:
        send_part(part, d, e_recv)
    for b, where in PRE:
        if b in early:
            def issue():
                for d in [across(k) for k in range(side)] if where == 'a' else [beside(k) for k in range(1, side)]:
                    post(b, d)
            from_us(b, issue)

    load_owners.wait()

    @pl.loop(0, blocks)
    def _(o):
        found = jnp.int32(0)
        for b in range(blocks):
            found = jnp.where(owners[b] == o, jnp.int32(b), found)
        inverse[o] = found

    for b in early:
        keep(b)
    energies(groups - 1, e_recv).wait_recv()
    total = parts[0]
    for g in range(1, groups):
        total = total + parts[g]
    energy = jnp.sum(jnp.where(own_lanes, total, 0.0), axis=1, keepdims=True)
    scale = 1.0 / jnp.sqrt(energy * (1.0 / (tokens * groups * features)) + 1.0)

    def fill(b):
        _, piece, low, high, _, _ = boxes[b]
        for d in range(groups):
            chunk, tile = divmod(d * each + piece, row_tiles)
            for j in range(low, high):
                late[b][0, d * (high - low) + j - low] = (centered[tile, chunk, j] * scale).astype(jnp.bfloat16)

    def finish(who):
        ours = [b for b in late if boxes[b][5] in (None, who)]
        for b in ours:
            fill(b)
        for d in around:
            for b in ours:
                post(b, d)

    if any(boxes[b][5] is not None for b in late):
        for who in range(2):
            pl.when(upper == who)(functools.partial(finish, who))
    elif late:
        finish(None)
    for b in late:
        keep(b)

    def span_of(b, count):
        wanted, raw = count * (boxes[b][3] - boxes[b][2]), boxes[b][4]
        model = b if wanted <= r1[b].shape[1] else next(
            m for m in range(nb) if boxes[m][4] == raw and r1[m].shape[0] == 1 and r1[m].shape[1] >= wanted)
        return r1[model].at[:, pl.ds(0, wanted)]

    def arrival(b, count):
        span = span_of(b, count)
        return pltpu.make_async_remote_copy(
            src_ref=span, dst_ref=span, send_sem=send1.at[b], recv_sem=recv1.at[b],
            device_id=(section, group), device_id_type=MESH)

    def await_box(b):
        half, _, _, _, _, who = boxes[b]
        if who is None:
            arrival(b, (side if half else groups) - 1).wait_recv()
        else:
            pl.when(upper == who)(lambda: arrival(b, side - 1).wait_recv())
            pl.when(upper != who)(lambda: arrival(b, side).wait_recv())

    def await_sent(b):
        from_us(b, lambda: arrival(b, (side if boxes[b][0] else groups) - 1).wait_send())

    def delivered(u):
        span = r2[u].at[pl.ds(0, sections * groups - 1)]
        return pltpu.make_async_remote_copy(
            src_ref=span, dst_ref=span, send_sem=send2.at[u], recv_sem=recv2.at[u],
            device_id=(section, group), device_id_type=MESH)

    def boxes_of(piece):
        return [b for b in range(nb) if boxes[b][1] == piece and not boxes[b][0]]

    def needs(u):
        return [0] if u == 0 else [b for piece in (units[u] if u > 1 else [0]) for b in boxes_of(piece)]

    def scaled(v):
        return (v * scale).astype(jnp.bfloat16)

    def take(u, o):
        at = inverse[o]
        if u == 0:
            at = lax.rem(at, side * per_dev)
            return [scaled(r1[0][tile, at]) for tile in range(row_tiles)]
        if u == 1:
            return [scaled(r1[1][0, at])]
        got = []
        for piece in units[u]:
            which = boxes_of(piece)
            if len(which) == 1:
                got.append(r1[which[0]][0, at])
            else:
                cut = boxes[which[0]][3]
                d, j = at // per_dev, lax.rem(at, per_dev)
                place = lax.rem(d, side)
                first = scaled(r1[which[0]][0, place * cut + lax.rem(j, cut)])
                second = r1[which[1]][0, place * (per_dev - cut) + lax.rem(j, per_dev - cut)]
                third = r1[which[2]][0, place * per_dev + j]
                got.append(jnp.where(d // side == WHO, jnp.where(j < cut, first, second), third))
        return got

    def deliver(u, planes):
        keys = [(h, c, q) for q in range(sections) for h in range(quarter // 2) for c in range(2)]
        routes = []
        for t in planes:
            t, part = t if isinstance(t, tuple) else (t, None)
            routes += [(t, k, k[2]) for k in keys if part is None or (part == 'a') == (k[0] == 0 and k[2] == 0)]
        by_plane = {}
        for r in routes:
            by_plane.setdefault(r[0], []).append(r)
        routes = [r for n in range(len(keys)) for rs in by_plane.values() for r in rs[n:n + 1]]

        def place(t, k, q):
            h, c, _ = k
            sec, d = jnp.int32(q), t * quarter + h * 2 + lax.rem(corner + c, 2)
            return sec, d, sec * groups + d

        def select(t, k, q):
            o = place(t, k, q)[2]
            for tile, block in enumerate(take(u, o)):
                s2[u][o, tile] = block

        def send(t, k, q):
            sec, d, o = place(t, k, q)

            def go():
                pltpu.make_async_remote_copy(
                    src_ref=s2[u].at[o], dst_ref=r2[u].at[me], send_sem=send2.at[u], recv_sem=recv2.at[u],
                    device_id=(sec, d), device_id_type=MESH).start()
            h, c, _ = k
            if c:
                go()
            else:
                pl.when((plane != t) | (section != q) | (corner // 2 != h))(go)

        for n in range(len(routes) + LAG):
            if n < len(routes):
                select(*routes[n])
            if n >= LAG:
                send(*routes[n - LAG])

    steps = STEPS if nu == max(u for u, _ in STEPS) + 1 else [(u, (0, 1, 2, 3)) for u in range(nu)]
    seen = []
    for u, planes in steps:
        if u not in seen:
            for b in needs(u):
                await_box(b)
            seen.append(u)
        deliver(u, planes)
    for u in seen:
        for tile, block in enumerate(take(u, me)):
            r2[u][me, tile] = block
    order = seen

    home = inverse[me] // (side * per_dev) * side

    def assemble(tile, chunk, got):
        for i in range(per_tile):
            out_ref[tile * per_tile + i, :, chunk * LANES:(chunk + 1) * LANES] = jnp.concatenate(
                [v[i * layers:(i + 1) * layers] for v in got], axis=0).astype(jnp.bfloat16)

    for u in order:
        delivered(u).wait_recv()
        if u == 0:
            for d in range(side):
                for tile in range(row_tiles):
                    assemble(tile, wide_chunks + d,
                             [r2[u][s * groups + home + d, tile].astype(jnp.float32) for s in range(sections)])
        else:
            for d in range(groups):
                for n, piece in enumerate(units[u] if u > 1 else [0]):
                    chunk, tile = divmod(d * each + piece, row_tiles)
                    assemble(tile, chunk, [r2[u][s * groups + d, n].astype(jnp.float32) for s in range(sections)])

    energies(groups - 1, e_recv).wait_send()
    for b in range(nb):
        await_sent(b)
    for u in range(nu):
        delivered(u).wait_send()


def store_kernel(assembled, out_hbm, sem):
    store = pltpu.make_async_copy(assembled, out_hbm, sem)
    store.start()
    store.wait()


def solution(mesh):
    sections, groups = mesh.shape["section"], mesh.shape["dp"]

    def on_device(residuals, owners):
        layers, tokens, features = residuals.shape
        blocks = owners.shape[0]
        per_dev = blocks // groups
        block_len = tokens // per_dev
        row_tiles = block_len * layers // SUBLANES
        pieces, side = features // LANES * row_tiles, groups // 2
        each = (pieces - row_tiles * side) // groups
        boxes, units = layout(row_tiles, per_dev, each)
        tile = (SUBLANES, LANES)
        dma = pltpu.SemaphoreType.DMA
        inboxes = [(row_tiles if half else 1, (side if half or who is not None else groups) * (high - low), *tile)
                   for half, _, low, high, _, who in boxes]
        outboxes = [(blocks, row_tiles if u == 0 else 1 if u == 1 else len(units[u]), *tile) for u in range(len(units))]
        received = pl.pallas_call(
            functools.partial(harvest_kernel, sections, groups, each),
            out_shape=pltpu.VMEM((block_len, layers * sections, features), jnp.bfloat16),
            in_specs=[pl.BlockSpec(memory_space=pl.ANY), pl.BlockSpec(memory_space=pl.ANY)],
            out_specs=pl.BlockSpec(memory_space=pltpu.VMEM),
            scratch_shapes=[
                pltpu.SMEM((blocks,), jnp.int32),
                pltpu.SMEM((blocks,), jnp.int32),
                pltpu.VMEM((layers, tokens, features), jnp.float32),
                pltpu.VMEM((row_tiles, features // LANES, per_dev, *tile), jnp.float32),
                pltpu.VMEM((1, LANES), jnp.float32),
                pltpu.VMEM((groups, 1, LANES), jnp.float32),
                dma, dma, dma, dma,
                *[dma((len(boxes),)) for _ in range(2)],
                *[dma((len(units),)) for _ in range(2)],
                *[pltpu.VMEM(inboxes[b], jnp.float32 if boxes[b][4] else jnp.bfloat16) for b in range(len(boxes))],
                *[pltpu.VMEM(shape, jnp.bfloat16) for shape in outboxes * 2],
                *[pltpu.VMEM((1, groups * (b[3] - b[2]), *tile), jnp.bfloat16) for b in boxes if not b[4]],
            ],
            compiler_params=pltpu.CompilerParams(collective_id=0, has_side_effects=True),
            name="harvest",
        )(residuals, owners)
        return pl.pallas_call(
            store_kernel,
            out_shape=jax.ShapeDtypeStruct(received.shape, received.dtype),
            in_specs=[pl.BlockSpec(memory_space=pltpu.VMEM)],
            out_specs=pl.BlockSpec(memory_space=pl.ANY),
            scratch_shapes=[pltpu.SemaphoreType.DMA],
            name="store",
        )(pltpu.with_memory_space_constraint(received, pltpu.VMEM))

    in_specs = (P("section", "dp", None), P())
    out_specs = P(("section", "dp"), None, None)
    return jax.shard_map(on_device, mesh=mesh, in_specs=in_specs, out_specs=out_specs, check_vma=False)
```

```python
import functools

import jax
import jax.numpy as jnp
from jax import lax
from jax.experimental import pallas as pl
from jax.experimental.pallas import tpu as pltpu
from jax.sharding import PartitionSpec as P

MESH = pl.DeviceIdType.MESH
LANES = 128
SUBLANES = 8
LAG = 8
SHARE = 2
WHO = 1
PRE = ((1, 'a'), (0, 'b'), (1, 'b'), (2, 'a'), (2, 'b'))
STEPS = ((0, (0, 2)), (1, (0, 2, 3)), (0, ((1, 'a'), 3)), (1, ((1, 'a'),)), (2, (0, 2, 3)), (2, ((1, 'a'),)), (0, ((1, 'b'),)), (1, ((1, 'b'),)), (2, ((1, 'b'),)))


def layout(row_tiles, per_dev, each):
    share = per_dev // SHARE
    boxes = [(True, None, 0, per_dev, True, None), (False, 0, 0, per_dev, True, None)]
    for piece in range(1, each):
        cut = share if piece == 1 else 0
        if cut:
            boxes.append((False, piece, 0, cut, True, WHO))
            boxes.append((False, piece, cut, per_dev, False, WHO))
            boxes.append((False, piece, 0, per_dev, False, 1 - WHO))
        else:
            boxes.append((False, piece, 0, per_dev, False, None))
    units = [[0], [1]] + ([list(range(1, each))] if each > 1 else [])
    return boxes, units


def harvest_kernel(sections, groups, each, x_hbm, owners_hbm, out_ref, owners, inverse, xv, centered, part,
                   parts, x_sem, o_sem, e_send, e_recv, send1, recv1, send2, recv2, *buffers):
    layers, tokens, features = x_hbm.shape
    pieces = features // LANES
    blocks = owners.shape[0]
    per_dev = blocks // groups
    side, quarter = groups // 2, groups // 4
    row_tiles = centered.shape[0]
    wide_chunks = groups * each // row_tiles
    boxes, units = layout(row_tiles, per_dev, each)
    nb, nu = len(boxes), len(units)
    r1, s2, r2, late = buffers[:nb], buffers[nb:nb + nu], buffers[nb + nu:nb + 2 * nu], buffers[nb + 2 * nu:]
    late = dict(zip([b for b in range(nb) if not boxes[b][4]], late))
    section, group = lax.axis_index("section"), lax.axis_index("dp")
    me = section * groups + group
    upper = group // side
    spot, base = lax.rem(group, side), upper * side

    load = pltpu.make_async_copy(x_hbm, xv, x_sem)
    load.start()
    load_owners = pltpu.make_async_copy(owners_hbm, owners, o_sem)
    load_owners.start()
    barrier = pltpu.get_barrier_semaphore()

    def peer_of(p):
        return lax.rem(group + p, groups)

    def beside(k):
        return base + lax.rem(spot + k, side)

    def across(k):
        return side - base + lax.rem(spot + k, side)

    def signal(sem, d):
        pl.semaphore_signal(sem, inc=1, device_id=(section, d), device_id_type=MESH)

    plane, corner = group // quarter, lax.rem(group, quarter)

    def member(t, k):
        return t * quarter + lax.rem(corner + k, quarter)

    for t in range(4):
        for k in range(quarter):
            if k:
                signal(barrier, member(t, k))
            else:
                pl.when(plane != t)(lambda: signal(barrier, member(t, k)))
    for k in range(1, sections):
        pl.semaphore_signal(barrier, inc=1, device_id=(lax.rem(section + k, sections), group), device_id_type=MESH)

    load.wait()
    per_tile = SUBLANES // layers
    lane = lax.broadcasted_iota(jnp.int32, (SUBLANES, LANES), 1)
    row = lax.broadcasted_iota(jnp.int32, (SUBLANES, LANES), 0)
    total = jnp.zeros((SUBLANES, LANES), jnp.float32)
    for l in range(layers):
        acc = jnp.zeros((SUBLANES, LANES), jnp.float32)
        for t in range(0, tokens, SUBLANES):
            x = xv[l, t:t + SUBLANES]
            c = x - jnp.sum(x, axis=1, keepdims=True) * (1.0 / features)
            xv[l, t:t + SUBLANES] = c
            sq = c * c
            for f in range(pieces):
                acc = acc + sq[:, f * LANES:(f + 1) * LANES]
        fold = LANES // 2
        while fold >= LANES // layers:
            acc = acc + pltpu.roll(acc, fold, 1)
            fold //= 2
        total = total + jnp.where(lane // (LANES // layers) == l, acc, 0.0)
    own_lanes = lane // (LANES // layers) == row % layers
    acc = jnp.sum(total, axis=0, keepdims=True)
    part[...] = acc
    parts[group] = acc

    for g in range(tokens // per_tile):
        j, tile = divmod(g, row_tiles)
        c = jnp.concatenate([xv[:, g * per_tile + i, :] for i in range(per_tile)], axis=0)
        for f in range(pieces):
            centered[tile, f, j] = c[:, f * LANES:(f + 1) * LANES]

    def send_part(source, d, sem):
        pltpu.make_async_remote_copy(
            src_ref=source, dst_ref=parts.at[group], send_sem=e_send, recv_sem=sem,
            device_id=(section, d), device_id_type=MESH).start()

    def energies(count, sem):
        span = parts.at[pl.ds(0, count)]
        return pltpu.make_async_remote_copy(
            src_ref=span, dst_ref=span, send_sem=e_send, recv_sem=sem,
            device_id=(section, group), device_id_type=MESH)

    def source(b, d):
        half, piece, low, high, raw, _ = boxes[b]
        if half:
            return centered.at[:, wide_chunks + lax.rem(d, side)]
        if not raw:
            return late[b].at[:, pl.ds(d * (high - low), high - low)]
        at = d * each + piece
        return centered.at[pl.ds(lax.rem(at, row_tiles), 1), at // row_tiles, pl.ds(low, high - low)]

    def slot(b):
        half, _, low, high, _, who = boxes[b]
        return pl.ds((spot if half or who is not None else group) * (high - low), high - low)

    def from_us(b, body):
        who = boxes[b][5]
        if who is None:
            body()
        else:
            pl.when(upper == who)(body)

    def post(b, d):
        pltpu.make_async_remote_copy(
            src_ref=source(b, d), dst_ref=r1[b].at[:, slot(b)], send_sem=send1.at[b], recv_sem=recv1.at[b],
            device_id=(section, d), device_id_type=MESH).start()

    def keep(b):
        def body():
            r1[b][:, slot(b)] = source(b, group)[...]
        from_us(b, body)

    around = [peer_of(p) for p in sorted(range(1, groups), key=lambda p: min(p, groups - p))]

    early = [b for b in range(nb) if boxes[b][4]]

    pl.semaphore_wait(barrier, groups + sections - 2)
    for d in around:
        send_part(part, d, e_recv)
    for b, where in PRE:
        if b in early:
            def issue():
                for d in [across(k) for k in range(side)] if where == 'a' else [beside(k) for k in range(1, side)]:
                    post(b, d)
            from_us(b, issue)

    load_owners.wait()

    @pl.loop(0, blocks)
    def _(o):
        found = jnp.int32(0)
        for b in range(blocks):
            found = jnp.where(owners[b] == o, jnp.int32(b), found)
        inverse[o] = found

    for b in early:
        keep(b)
    energies(groups - 1, e_recv).wait_recv()
    total = parts[0]
    for g in range(1, groups):
        total = total + parts[g]
    energy = jnp.sum(jnp.where(own_lanes, total, 0.0), axis=1, keepdims=True)
    scale = 1.0 / jnp.sqrt(energy * (1.0 / (tokens * groups * features)) + 1.0)

    def fill(b):
        _, piece, low, high, _, _ = boxes[b]
        for d in range(groups):
            chunk, tile = divmod(d * each + piece, row_tiles)
            for j in range(low, high):
                late[b][0, d * (high - low) + j - low] = (centered[tile, chunk, j] * scale).astype(jnp.bfloat16)

    def finish(who):
        ours = [b for b in late if boxes[b][5] in (None, who)]
        for b in ours:
            fill(b)
        order = around
        if who == 0:
            order = [across(k) for k in range(side)] + [beside(k) for k in range(1, side)]
        for d in order:
            for b in ours:
                post(b, d)

    if any(boxes[b][5] is not None for b in late):
        for who in range(2):
            pl.when(upper == who)(functools.partial(finish, who))
    elif late:
        finish(None)
    for b in late:
        keep(b)

    def span_of(b, count):
        wanted, raw = count * (boxes[b][3] - boxes[b][2]), boxes[b][4]
        model = b if wanted <= r1[b].shape[1] else next(
            m for m in range(nb) if boxes[m][4] == raw and r1[m].shape[0] == 1 and r1[m].shape[1] >= wanted)
        return r1[model].at[:, pl.ds(0, wanted)]

    def arrival(b, count):
        span = span_of(b, count)
        return pltpu.make_async_remote_copy(
            src_ref=span, dst_ref=span, send_sem=send1.at[b], recv_sem=recv1.at[b],
            device_id=(section, group), device_id_type=MESH)

    def await_box(b):
        half, _, _, _, _, who = boxes[b]
        if who is None:
            arrival(b, (side if half else groups) - 1).wait_recv()
        else:
            pl.when(upper == who)(lambda: arrival(b, side - 1).wait_recv())
            pl.when(upper != who)(lambda: arrival(b, side).wait_recv())

    def await_sent(b):
        from_us(b, lambda: arrival(b, (side if boxes[b][0] else groups) - 1).wait_send())

    def delivered(u):
        span = r2[u].at[pl.ds(0, sections * groups - 1)]
        return pltpu.make_async_remote_copy(
            src_ref=span, dst_ref=span, send_sem=send2.at[u], recv_sem=recv2.at[u],
            device_id=(section, group), device_id_type=MESH)

    def boxes_of(piece):
        return [b for b in range(nb) if boxes[b][1] == piece and not boxes[b][0]]

    def needs(u):
        return [0] if u == 0 else [b for piece in (units[u] if u > 1 else [0]) for b in boxes_of(piece)]

    def scaled(v):
        return (v * scale).astype(jnp.bfloat16)

    def take(u, o):
        at = inverse[o]
        if u == 0:
            at = lax.rem(at, side * per_dev)
            return [scaled(r1[0][tile, at]) for tile in range(row_tiles)]
        if u == 1:
            return [scaled(r1[1][0, at])]
        got = []
        for piece in units[u]:
            which = boxes_of(piece)
            if len(which) == 1:
                got.append(r1[which[0]][0, at])
            else:
                cut = boxes[which[0]][3]
                d, j = at // per_dev, lax.rem(at, per_dev)
                place = lax.rem(d, side)
                first = scaled(r1[which[0]][0, place * cut + lax.rem(j, cut)])
                second = r1[which[1]][0, place * (per_dev - cut) + lax.rem(j, per_dev - cut)]
                third = r1[which[2]][0, place * per_dev + j]
                got.append(jnp.where(d // side == WHO, jnp.where(j < cut, first, second), third))
        return got

    def deliver(u, planes):
        keys = [(h, c, q) for q in range(sections) for h in range(quarter // 2) for c in range(2)]
        routes = []
        for t in planes:
            t, part = t if isinstance(t, tuple) else (t, None)
            routes += [(t, k, k[2]) for k in keys if part is None or (part == 'a') == (k[0] == 0 and k[2] == 0)]
        by_plane = {}
        for r in routes:
            by_plane.setdefault(r[0], []).append(r)
        routes = [r for n in range(len(keys)) for rs in by_plane.values() for r in rs[n:n + 1]]

        def place(t, k, q):
            h, c, _ = k
            sec, d = jnp.int32(q), t * quarter + h * 2 + lax.rem(corner + c, 2)
            return sec, d, sec * groups + d

        def select(t, k, q):
            o = place(t, k, q)[2]
            for tile, block in enumerate(take(u, o)):
                s2[u][o, tile] = block

        def send(t, k, q):
            sec, d, o = place(t, k, q)

            def go():
                pltpu.make_async_remote_copy(
                    src_ref=s2[u].at[o], dst_ref=r2[u].at[me], send_sem=send2.at[u], recv_sem=recv2.at[u],
                    device_id=(sec, d), device_id_type=MESH).start()
            h, c, _ = k
            if c:
                go()
            else:
                pl.when((plane != t) | (section != q) | (corner // 2 != h))(go)

        for n in range(len(routes) + LAG):
            if n < len(routes):
                select(*routes[n])
            if n >= LAG:
                send(*routes[n - LAG])

    steps = STEPS if nu == max(u for u, _ in STEPS) + 1 else [(u, (0, 1, 2, 3)) for u in range(nu)]
    seen = []
    for u, planes in steps:
        if u not in seen:
            for b in needs(u):
                await_box(b)
            seen.append(u)
        deliver(u, planes)
    for u in seen:
        for tile, block in enumerate(take(u, me)):
            r2[u][me, tile] = block
    order = seen

    home = inverse[me] // (side * per_dev) * side

    def assemble(tile, chunk, got):
        for i in range(per_tile):
            out_ref[tile * per_tile + i, :, chunk * LANES:(chunk + 1) * LANES] = jnp.concatenate(
                [v[i * layers:(i + 1) * layers] for v in got], axis=0).astype(jnp.bfloat16)

    for u in order:
        delivered(u).wait_recv()
        if u == 0:
            for d in range(side):
                for tile in range(row_tiles):
                    assemble(tile, wide_chunks + d,
                             [r2[u][s * groups + home + d, tile].astype(jnp.float32) for s in range(sections)])
        else:
            for d in range(groups):
                for n, piece in enumerate(units[u] if u > 1 else [0]):
                    chunk, tile = divmod(d * each + piece, row_tiles)
                    assemble(tile, chunk, [r2[u][s * groups + d, n].astype(jnp.float32) for s in range(sections)])

    energies(groups - 1, e_recv).wait_send()
    for b in range(nb):
        await_sent(b)
    for u in range(nu):
        delivered(u).wait_send()


def store_kernel(assembled, out_hbm, sem):
    store = pltpu.make_async_copy(assembled, out_hbm, sem)
    store.start()
    store.wait()


def solution(mesh):
    sections, groups = mesh.shape["section"], mesh.shape["dp"]

    def on_device(residuals, owners):
        layers, tokens, features = residuals.shape
        blocks = owners.shape[0]
        per_dev = blocks // groups
        block_len = tokens // per_dev
        row_tiles = block_len * layers // SUBLANES
        pieces, side = features // LANES * row_tiles, groups // 2
        each = (pieces - row_tiles * side) // groups
        boxes, units = layout(row_tiles, per_dev, each)
        tile = (SUBLANES, LANES)
        dma = pltpu.SemaphoreType.DMA
        inboxes = [(row_tiles if half else 1, (side if half or who is not None else groups) * (high - low), *tile)
                   for half, _, low, high, _, who in boxes]
        outboxes = [(blocks, row_tiles if u == 0 else 1 if u == 1 else len(units[u]), *tile) for u in range(len(units))]
        received = pl.pallas_call(
            functools.partial(harvest_kernel, sections, groups, each),
            out_shape=pltpu.VMEM((block_len, layers * sections, features), jnp.bfloat16),
            in_specs=[pl.BlockSpec(memory_space=pl.ANY), pl.BlockSpec(memory_space=pl.ANY)],
            out_specs=pl.BlockSpec(memory_space=pltpu.VMEM),
            scratch_shapes=[
                pltpu.SMEM((blocks,), jnp.int32),
                pltpu.SMEM((blocks,), jnp.int32),
                pltpu.VMEM((layers, tokens, features), jnp.float32),
                pltpu.VMEM((row_tiles, features // LANES, per_dev, *tile), jnp.float32),
                pltpu.VMEM((1, LANES), jnp.float32),
                pltpu.VMEM((groups, 1, LANES), jnp.float32),
                dma, dma, dma, dma,
                *[dma((len(boxes),)) for _ in range(2)],
                *[dma((len(units),)) for _ in range(2)],
                *[pltpu.VMEM(inboxes[b], jnp.float32 if boxes[b][4] else jnp.bfloat16) for b in range(len(boxes))],
                *[pltpu.VMEM(shape, jnp.bfloat16) for shape in outboxes * 2],
                *[pltpu.VMEM((1, groups * (b[3] - b[2]), *tile), jnp.bfloat16) for b in boxes if not b[4]],
            ],
            compiler_params=pltpu.CompilerParams(collective_id=0, has_side_effects=True),
            name="harvest",
        )(residuals, owners)
        return pl.pallas_call(
            store_kernel,
            out_shape=jax.ShapeDtypeStruct(received.shape, received.dtype),
            in_specs=[pl.BlockSpec(memory_space=pltpu.VMEM)],
            out_specs=pl.BlockSpec(memory_space=pl.ANY),
            scratch_shapes=[pltpu.SemaphoreType.DMA],
            name="store",
        )(pltpu.with_memory_space_constraint(received, pltpu.VMEM))

    in_specs = (P("section", "dp", None), P())
    out_specs = P(("section", "dp"), None, None)
    return jax.shard_map(on_device, mesh=mesh, in_specs=in_specs, out_specs=out_specs, check_vma=False)
```

```python
import functools

import jax
import jax.numpy as jnp
from jax import lax
from jax.experimental import pallas as pl
from jax.experimental.pallas import tpu as pltpu
from jax.sharding import PartitionSpec as P

MESH = pl.DeviceIdType.MESH
LANES = 128
SUBLANES = 8
LAG = 8
SHARE = 2
WHO = 1
PRE = ((1, 'a'), (0, 'b'), (1, 'b'), (2, 'a'), (2, 'b'))
STEPS = ((0, (0, 2)), (1, (0, 2, 3)), (0, ((1, 'a'), 3)), (1, ((1, 'a'),)), (2, (0, 2, 3)), (2, ((1, 'a'),)), (0, ((1, 'b'),)), (1, ((1, 'b'),)), (2, ((1, 'b'),)))


def layout(row_tiles, per_dev, each):
    share = per_dev // SHARE
    boxes = [(True, None, 0, per_dev, True, None), (False, 0, 0, per_dev, True, None)]
    for piece in range(1, each):
        cut = share if piece == 1 else 0
        if cut:
            boxes.append((False, piece, 0, cut, True, WHO))
            boxes.append((False, piece, cut, per_dev, False, WHO))
            boxes.append((False, piece, 0, per_dev, False, 1 - WHO))
        else:
            boxes.append((False, piece, 0, per_dev, False, None))
    units = [[0], [1]] + ([list(range(1, each))] if each > 1 else [])
    return boxes, units


def harvest_kernel(sections, groups, each, x_hbm, owners_hbm, out_ref, owners, inverse, xv, centered, part,
                   parts, x_sem, o_sem, e_send, e_recv, send1, recv1, send2, recv2, *buffers):
    layers, tokens, features = x_hbm.shape
    pieces = features // LANES
    blocks = owners.shape[0]
    per_dev = blocks // groups
    side, quarter = groups // 2, groups // 4
    row_tiles = centered.shape[0]
    wide_chunks = groups * each // row_tiles
    boxes, units = layout(row_tiles, per_dev, each)
    nb, nu = len(boxes), len(units)
    r1, s2, r2, late = buffers[:nb], buffers[nb:nb + nu], buffers[nb + nu:nb + 2 * nu], buffers[nb + 2 * nu:]
    late = dict(zip([b for b in range(nb) if not boxes[b][4]], late))
    section, group = lax.axis_index("section"), lax.axis_index("dp")
    me = section * groups + group
    upper = group // side
    spot, base = lax.rem(group, side), upper * side

    load = pltpu.make_async_copy(x_hbm, xv, x_sem)
    load.start()
    load_owners = pltpu.make_async_copy(owners_hbm, owners, o_sem)
    load_owners.start()
    barrier = pltpu.get_barrier_semaphore()

    def peer_of(p):
        return lax.rem(group + p, groups)

    def beside(k):
        return base + lax.rem(spot + k, side)

    def across(k):
        return side - base + lax.rem(spot + k, side)

    def signal(sem, d):
        pl.semaphore_signal(sem, inc=1, device_id=(section, d), device_id_type=MESH)

    plane, corner = group // quarter, lax.rem(group, quarter)

    def member(t, k):
        return t * quarter + lax.rem(corner + k, quarter)

    for t in range(4):
        for k in range(quarter):
            if k:
                signal(barrier, member(t, k))
            else:
                pl.when(plane != t)(lambda: signal(barrier, member(t, k)))
    for k in range(1, sections):
        pl.semaphore_signal(barrier, inc=1, device_id=(lax.rem(section + k, sections), group), device_id_type=MESH)

    load.wait()
    per_tile = SUBLANES // layers
    lane = lax.broadcasted_iota(jnp.int32, (SUBLANES, LANES), 1)
    row = lax.broadcasted_iota(jnp.int32, (SUBLANES, LANES), 0)
    total = jnp.zeros((SUBLANES, LANES), jnp.float32)
    for l in range(layers):
        acc = jnp.zeros((SUBLANES, LANES), jnp.float32)
        for t in range(0, tokens, SUBLANES):
            x = xv[l, t:t + SUBLANES]
            c = x - jnp.sum(x, axis=1, keepdims=True) * (1.0 / features)
            xv[l, t:t + SUBLANES] = c
            sq = c * c
            for f in range(pieces):
                acc = acc + sq[:, f * LANES:(f + 1) * LANES]
        fold = LANES // 2
        while fold >= LANES // layers:
            acc = acc + pltpu.roll(acc, fold, 1)
            fold //= 2
        total = total + jnp.where(lane // (LANES // layers) == l, acc, 0.0)
    own_lanes = lane // (LANES // layers) == row % layers
    acc = jnp.sum(total, axis=0, keepdims=True)
    part[...] = acc
    parts[group] = acc

    for g in range(tokens // per_tile):
        j, tile = divmod(g, row_tiles)
        c = jnp.concatenate([xv[:, g * per_tile + i, :] for i in range(per_tile)], axis=0)
        for f in range(pieces):
            centered[tile, f, j] = c[:, f * LANES:(f + 1) * LANES]

    def send_part(source, d, sem):
        pltpu.make_async_remote_copy(
            src_ref=source, dst_ref=parts.at[group], send_sem=e_send, recv_sem=sem,
            device_id=(section, d), device_id_type=MESH).start()

    def energies(count, sem):
        span = parts.at[pl.ds(0, count)]
        return pltpu.make_async_remote_copy(
            src_ref=span, dst_ref=span, send_sem=e_send, recv_sem=sem,
            device_id=(section, group), device_id_type=MESH)

    def source(b, d):
        half, piece, low, high, raw, _ = boxes[b]
        if half:
            return centered.at[:, wide_chunks + lax.rem(d, side)]
        if not raw:
            return late[b].at[:, pl.ds(d * (high - low), high - low)]
        at = d * each + piece
        return centered.at[pl.ds(lax.rem(at, row_tiles), 1), at // row_tiles, pl.ds(low, high - low)]

    def slot(b):
        half, _, low, high, _, who = boxes[b]
        return pl.ds((spot if half or who is not None else group) * (high - low), high - low)

    def from_us(b, body):
        who = boxes[b][5]
        if who is None:
            body()
        else:
            pl.when(upper == who)(body)

    def post(b, d):
        pltpu.make_async_remote_copy(
            src_ref=source(b, d), dst_ref=r1[b].at[:, slot(b)], send_sem=send1.at[b], recv_sem=recv1.at[b],
            device_id=(section, d), device_id_type=MESH).start()

    def keep(b):
        def body():
            r1[b][:, slot(b)] = source(b, group)[...]
        from_us(b, body)

    around = [peer_of(p) for p in sorted(range(1, groups), key=lambda p: min(p, groups - p))]

    early = [b for b in range(nb) if boxes[b][4]]

    pl.semaphore_wait(barrier, groups + sections - 2)
    for d in around:
        send_part(part, d, e_recv)
    for b, where in PRE:
        if b in early:
            def issue():
                for d in [across(k) for k in range(side)] if where == 'a' else [beside(k) for k in range(1, side)]:
                    post(b, d)
            from_us(b, issue)

    load_owners.wait()

    @pl.loop(0, blocks)
    def _(o):
        found = jnp.int32(0)
        for b in range(blocks):
            found = jnp.where(owners[b] == o, jnp.int32(b), found)
        inverse[o] = found

    for b in early:
        keep(b)
    energies(groups - 1, e_recv).wait_recv()
    total = parts[0]
    for g in range(1, groups):
        total = total + parts[g]
    energy = jnp.sum(jnp.where(own_lanes, total, 0.0), axis=1, keepdims=True)
    scale = 1.0 / jnp.sqrt(energy * (1.0 / (tokens * groups * features)) + 1.0)

    def fill(b):
        _, piece, low, high, _, _ = boxes[b]
        for d in range(groups):
            chunk, tile = divmod(d * each + piece, row_tiles)
            for j in range(low, high):
                late[b][0, d * (high - low) + j - low] = (centered[tile, chunk, j] * scale).astype(jnp.bfloat16)

    def finish(who):
        ours = [b for b in late if boxes[b][5] in (None, who)]
        for b in ours:
            fill(b)
        order = around
        if who == 0:
            order = [member(t, k) for t in (3, 2) for k in range(quarter)] + [beside(k) for k in range(1, side)]
        for d in order:
            for b in ours:
                post(b, d)

    if any(boxes[b][5] is not None for b in late):
        for who in range(2):
            pl.when(upper == who)(functools.partial(finish, who))
    elif late:
        finish(None)
    for b in late:
        keep(b)

    def span_of(b, count):
        wanted, raw = count * (boxes[b][3] - boxes[b][2]), boxes[b][4]
        model = b if wanted <= r1[b].shape[1] else next(
            m for m in range(nb) if boxes[m][4] == raw and r1[m].shape[0] == 1 and r1[m].shape[1] >= wanted)
        return r1[model].at[:, pl.ds(0, wanted)]

    def arrival(b, count):
        span = span_of(b, count)
        return pltpu.make_async_remote_copy(
            src_ref=span, dst_ref=span, send_sem=send1.at[b], recv_sem=recv1.at[b],
            device_id=(section, group), device_id_type=MESH)

    def await_box(b):
        half, _, _, _, _, who = boxes[b]
        if who is None:
            arrival(b, (side if half else groups) - 1).wait_recv()
        else:
            pl.when(upper == who)(lambda: arrival(b, side - 1).wait_recv())
            pl.when(upper != who)(lambda: arrival(b, side).wait_recv())

    def await_sent(b):
        from_us(b, lambda: arrival(b, (side if boxes[b][0] else groups) - 1).wait_send())

    def delivered(u):
        span = r2[u].at[pl.ds(0, sections * groups - 1)]
        return pltpu.make_async_remote_copy(
            src_ref=span, dst_ref=span, send_sem=send2.at[u], recv_sem=recv2.at[u],
            device_id=(section, group), device_id_type=MESH)

    def boxes_of(piece):
        return [b for b in range(nb) if boxes[b][1] == piece and not boxes[b][0]]

    def needs(u):
        return [0] if u == 0 else [b for piece in (units[u] if u > 1 else [0]) for b in boxes_of(piece)]

    def scaled(v):
        return (v * scale).astype(jnp.bfloat16)

    def take(u, o):
        at = inverse[o]
        if u == 0:
            at = lax.rem(at, side * per_dev)
            return [scaled(r1[0][tile, at]) for tile in range(row_tiles)]
        if u == 1:
            return [scaled(r1[1][0, at])]
        got = []
        for piece in units[u]:
            which = boxes_of(piece)
            if len(which) == 1:
                got.append(r1[which[0]][0, at])
            else:
                cut = boxes[which[0]][3]
                d, j = at // per_dev, lax.rem(at, per_dev)
                place = lax.rem(d, side)
                first = scaled(r1[which[0]][0, place * cut + lax.rem(j, cut)])
                second = r1[which[1]][0, place * (per_dev - cut) + lax.rem(j, per_dev - cut)]
                third = r1[which[2]][0, place * per_dev + j]
                got.append(jnp.where(d // side == WHO, jnp.where(j < cut, first, second), third))
        return got

    def deliver(u, planes):
        keys = [(h, c, q) for q in range(sections) for h in range(quarter // 2) for c in range(2)]
        routes = []
        for t in planes:
            t, part = t if isinstance(t, tuple) else (t, None)
            routes += [(t, k, k[2]) for k in keys if part is None or (part == 'a') == (k[0] == 0 and k[2] == 0)]
        by_plane = {}
        for r in routes:
            by_plane.setdefault(r[0], []).append(r)
        routes = [r for n in range(len(keys)) for rs in by_plane.values() for r in rs[n:n + 1]]

        def place(t, k, q):
            h, c, _ = k
            sec, d = jnp.int32(q), t * quarter + h * 2 + lax.rem(corner + c, 2)
            return sec, d, sec * groups + d

        def select(t, k, q):
            o = place(t, k, q)[2]
            for tile, block in enumerate(take(u, o)):
                s2[u][o, tile] = block

        def send(t, k, q):
            sec, d, o = place(t, k, q)

            def go():
                pltpu.make_async_remote_copy(
                    src_ref=s2[u].at[o], dst_ref=r2[u].at[me], send_sem=send2.at[u], recv_sem=recv2.at[u],
                    device_id=(sec, d), device_id_type=MESH).start()
            h, c, _ = k
            if c:
                go()
            else:
                pl.when((plane != t) | (section != q) | (corner // 2 != h))(go)

        for n in range(len(routes) + LAG):
            if n < len(routes):
                select(*routes[n])
            if n >= LAG:
                send(*routes[n - LAG])

    steps = STEPS if nu == max(u for u, _ in STEPS) + 1 else [(u, (0, 1, 2, 3)) for u in range(nu)]
    seen = []
    for u, planes in steps:
        if u not in seen:
            for b in needs(u):
                await_box(b)
            seen.append(u)
        deliver(u, planes)
    for u in seen:
        for tile, block in enumerate(take(u, me)):
            r2[u][me, tile] = block
    order = seen

    home = inverse[me] // (side * per_dev) * side

    def assemble(tile, chunk, got):
        for i in range(per_tile):
            out_ref[tile * per_tile + i, :, chunk * LANES:(chunk + 1) * LANES] = jnp.concatenate(
                [v[i * layers:(i + 1) * layers] for v in got], axis=0).astype(jnp.bfloat16)

    for u in order:
        delivered(u).wait_recv()
        if u == 0:
            for d in range(side):
                for tile in range(row_tiles):
                    assemble(tile, wide_chunks + d,
                             [r2[u][s * groups + home + d, tile].astype(jnp.float32) for s in range(sections)])
        else:
            for d in range(groups):
                for n, piece in enumerate(units[u] if u > 1 else [0]):
                    chunk, tile = divmod(d * each + piece, row_tiles)
                    assemble(tile, chunk, [r2[u][s * groups + d, n].astype(jnp.float32) for s in range(sections)])

    energies(groups - 1, e_recv).wait_send()
    for b in range(nb):
        await_sent(b)
    for u in range(nu):
        delivered(u).wait_send()


def store_kernel(assembled, out_hbm, sem):
    store = pltpu.make_async_copy(assembled, out_hbm, sem)
    store.start()
    store.wait()


def solution(mesh):
    sections, groups = mesh.shape["section"], mesh.shape["dp"]

    def on_device(residuals, owners):
        layers, tokens, features = residuals.shape
        blocks = owners.shape[0]
        per_dev = blocks // groups
        block_len = tokens // per_dev
        row_tiles = block_len * layers // SUBLANES
        pieces, side = features // LANES * row_tiles, groups // 2
        each = (pieces - row_tiles * side) // groups
        boxes, units = layout(row_tiles, per_dev, each)
        tile = (SUBLANES, LANES)
        dma = pltpu.SemaphoreType.DMA
        inboxes = [(row_tiles if half else 1, (side if half or who is not None else groups) * (high - low), *tile)
                   for half, _, low, high, _, who in boxes]
        outboxes = [(blocks, row_tiles if u == 0 else 1 if u == 1 else len(units[u]), *tile) for u in range(len(units))]
        received = pl.pallas_call(
            functools.partial(harvest_kernel, sections, groups, each),
            out_shape=pltpu.VMEM((block_len, layers * sections, features), jnp.bfloat16),
            in_specs=[pl.BlockSpec(memory_space=pl.ANY), pl.BlockSpec(memory_space=pl.ANY)],
            out_specs=pl.BlockSpec(memory_space=pltpu.VMEM),
            scratch_shapes=[
                pltpu.SMEM((blocks,), jnp.int32),
                pltpu.SMEM((blocks,), jnp.int32),
                pltpu.VMEM((layers, tokens, features), jnp.float32),
                pltpu.VMEM((row_tiles, features // LANES, per_dev, *tile), jnp.float32),
                pltpu.VMEM((1, LANES), jnp.float32),
                pltpu.VMEM((groups, 1, LANES), jnp.float32),
                dma, dma, dma, dma,
                *[dma((len(boxes),)) for _ in range(2)],
                *[dma((len(units),)) for _ in range(2)],
                *[pltpu.VMEM(inboxes[b], jnp.float32 if boxes[b][4] else jnp.bfloat16) for b in range(len(boxes))],
                *[pltpu.VMEM(shape, jnp.bfloat16) for shape in outboxes * 2],
                *[pltpu.VMEM((1, groups * (b[3] - b[2]), *tile), jnp.bfloat16) for b in boxes if not b[4]],
            ],
            compiler_params=pltpu.CompilerParams(collective_id=0, has_side_effects=True),
            name="harvest",
        )(residuals, owners)
        return pl.pallas_call(
            store_kernel,
            out_shape=jax.ShapeDtypeStruct(received.shape, received.dtype),
            in_specs=[pl.BlockSpec(memory_space=pltpu.VMEM)],
            out_specs=pl.BlockSpec(memory_space=pl.ANY),
            scratch_shapes=[pltpu.SemaphoreType.DMA],
            name="store",
        )(pltpu.with_memory_space_constraint(received, pltpu.VMEM))

    in_specs = (P("section", "dp", None), P())
    out_specs = P(("section", "dp"), None, None)
    return jax.shard_map(on_device, mesh=mesh, in_specs=in_specs, out_specs=out_specs, check_vma=False)
```
